8 devices in a mesh: ez: 2 (over z, y), ey: 2 (over x), ex: 2 (over core).
Axes of the slice: x: 2, y: 2, z: 1, core: 2. Of those that a mesh axis runs over, the one named last changes fastest.
Arguments:
- x_tokens: bfloat16 [512, 2048], P(('ez', 'ey', 'ex'))
- expert_ids: int32 [512, 8], P(('ez', 'ey', 'ex'))
- gate_vals: float32 [512, 8], P(('ez', 'ey', 'ex'))
- w_gate: bfloat16 [64, 2048, 1024], P(('ex', 'ey', 'ez'))
- w_up: bfloat16 [64, 2048, 1024], P(('ex', 'ey', 'ez'))
- w_down: bfloat16 [64, 1024, 2048], P(('ex', 'ey', 'ez'))
Outputs:
- output: bfloat16 [512, 2048], P(('ez', 'ey', 'ex'))
All inputs are finite; a program needn't handle non-finite values.
Results may differ from the reference program's by a relative error of at most 0.00108.
Values are sent between devices in bfloat16 or wider.
A program may use at most 1 GiB of HBM per device.

```python
import jax
import jax.numpy as jnp
from jax import lax

HIDDEN = 2048
FFN_DIM = 1024
EXPERTS = 64
TOP_K = 8
TOK_DEV = 64
DEVICES = 8
GROUPS = 8

TOKENS_ALL = DEVICES * TOK_DEV
CAP_EXPERT = 2 * DEVICES * TOK_DEV * TOP_K // EXPERTS


def draw_routing(route_key):
    perm_key, group_key = jax.random.split(route_key)
    group_size = EXPERTS // GROUPS
    pair_count = group_size // 2
    pick_groups = TOP_K // 2
    perm_score = jax.random.randint(perm_key, (DEVICES, GROUPS, group_size), 0, 1 << 20)
    inner_perm = jnp.argsort(perm_score * group_size + jnp.arange(group_size), axis=-1)
    inner_perm = inner_perm.at[:, :, 2].set(inner_perm[:, :, 0])
    group_score = jax.random.randint(group_key, (DEVICES, GROUPS), 0, 1 << 20)
    group_perm = jnp.argsort(group_score * GROUPS + jnp.arange(GROUPS), axis=-1)
    visit_idx = jnp.arange(TOK_DEV)[:, None] * pick_groups + jnp.arange(pick_groups)[None, :]
    dev_idx = jnp.arange(DEVICES)[:, None, None]
    group_id = group_perm[dev_idx, visit_idx[None] % GROUPS]
    pair_pos = 2 * ((visit_idx // GROUPS) % pair_count)[None]
    first_pick = inner_perm[dev_idx, group_id, pair_pos]
    second_pick = inner_perm[dev_idx, group_id, pair_pos + 1]
    local_pick = jnp.stack([first_pick, second_pick], axis=-1)
    expert_ids = group_id[:, :, :, None] * group_size + local_pick
    return expert_ids.reshape(TOKENS_ALL, TOP_K).astype(jnp.int32)


def setup_inputs(seed: int = 0) -> dict:
    base_key = jax.random.key(seed)
    key_x, key_gate, key_one, key_three, key_two, key_route = jax.random.split(base_key, 6)
    x_tokens = jax.random.normal(key_x, (TOKENS_ALL, HIDDEN), jnp.float32)
    gate_raw = jax.random.uniform(key_gate, (TOKENS_ALL, TOP_K), jnp.float32, 0.5, 1.5)
    gate_vals = 2.5 * gate_raw / jnp.sum(gate_raw, axis=1, keepdims=True)
    w_gate = jax.random.normal(key_one, (EXPERTS, HIDDEN, FFN_DIM), jnp.float32) * HIDDEN ** -0.5
    w_up = jax.random.normal(key_three, (EXPERTS, HIDDEN, FFN_DIM), jnp.float32) * HIDDEN ** -0.5
    w_down = jax.random.normal(key_two, (EXPERTS, FFN_DIM, HIDDEN), jnp.float32) * FFN_DIM ** -0.5
    return {
        'x_tokens': x_tokens.astype(jnp.bfloat16),
        'expert_ids': draw_routing(key_route),
        'gate_vals': gate_vals,
        'w_gate': w_gate.astype(jnp.bfloat16),
        'w_up': w_up.astype(jnp.bfloat16),
        'w_down': w_down.astype(jnp.bfloat16),
    }


def reference(x_tokens, expert_ids, gate_vals, w_gate, w_up, w_down):
    flat_ids = expert_ids.reshape(-1)
    flat_gates = gate_vals.reshape(-1)
    pair_tok = jnp.arange(TOKENS_ALL * TOP_K) // TOP_K
    slot_pos = jnp.arange(CAP_EXPERT)

    def expert_step(acc_sum, scan_in):
        expert, w_one, w_three, w_two = scan_in
        chosen = flat_ids == expert
        n_chosen = jnp.sum(chosen.astype(jnp.int32))
        pair_sel = jnp.nonzero(chosen, size=CAP_EXPERT, fill_value=0)[0]
        tok_sel = pair_tok[pair_sel]
        weight = jnp.where(slot_pos < n_chosen, flat_gates[pair_sel], 0.0)
        tok_rows = x_tokens[tok_sel]
        h_gate = jnp.dot(tok_rows, w_one, preferred_element_type=jnp.float32)
        h_up = jnp.dot(tok_rows, w_three, preferred_element_type=jnp.float32)
        act_bf = (jax.nn.silu(h_gate) * h_up).astype(jnp.bfloat16)
        exp_out = jnp.dot(act_bf, w_two, preferred_element_type=jnp.float32).astype(jnp.bfloat16)
        acc_sum = acc_sum.at[tok_sel].add(weight[:, None] * exp_out.astype(jnp.float32))
        return acc_sum, None

    acc_init = jnp.zeros((TOKENS_ALL, HIDDEN), jnp.float32)
    moe_sum = lax.scan(expert_step, acc_init, (jnp.arange(EXPERTS), w_gate, w_up, w_down))[0]
    return (x_tokens.astype(jnp.float32) + moe_sum).astype(jnp.bfloat16)
```

```python
import jax
import jax.numpy as jnp
from jax import lax
from jax.experimental import pallas as pl
from jax.experimental.pallas import tpu as pltpu
from jax.sharding import PartitionSpec as P

TOKEN_AXES = ('ez', 'ey', 'ex')
EXPERT_AXES = ('ex', 'ey', 'ez')
MESH = pl.DeviceIdType.MESH
F32 = jnp.float32
BF16 = jnp.bfloat16

TOK = 64
HID = 2048
FFN = 1024
NEXP = 8
CAP = 16
NSLOT = 10
CB = 256
NCB = HID // CB
N13 = 2 * NEXP

PEERS = [(c, s) for c in range(4) for s in range(2) if (c, s) != (0, 0)]


def kernel(x_hbm, ids_hbm, gates_hbm, wg_hbm, wu_hbm, wd_hbm, y_hbm,
           ring, xs, xe, act, acc, dsend, drecv, r2, f3, r3, pmat, gtmp, gmat, obuf, ids_v, gates_v, meta, yv,
           w_sem, loc_sem, xsend, xrecv, fsend, msend, mrecv, d_send, d_recv, s2_send, s2_recv, s3_send, s3_recv, y_sem):
    ez, ey, ex = lax.axis_index('ez'), lax.axis_index('ey'), lax.axis_index('ex')

    def dev(c, s):
        return (1 - ez if c & 2 else ez, 1 - ey if c & 1 else ey, 1 - ex if s else ex)

    def remote(src, dst, ssem, rsem, c, s):
        return pltpu.make_async_remote_copy(src_ref=src, dst_ref=dst, send_sem=ssem, recv_sem=rsem,
                                            device_id=dev(c, s), device_id_type=MESH)

    cp_x = pltpu.make_async_copy(x_hbm, xs.at[0, pl.ds(0, TOK)], loc_sem.at[0])
    cp_i = pltpu.make_async_copy(ids_hbm, ids_v, loc_sem.at[1])
    cp_g = pltpu.make_async_copy(gates_hbm, gates_v, loc_sem.at[2])
    cp_x.start()
    cp_i.start()
    cp_g.start()

    barrier = pltpu.get_barrier_semaphore()
    for c, s in PEERS:
        pl.semaphore_signal(barrier, inc=1, device_id=dev(c, s), device_id_type=MESH)

    def start_w13(w_hbm, e, slot):
        for q in range(4):
            pltpu.make_async_copy(w_hbm.at[e, :, :, pl.ds(q * CB, CB)], ring.at[slot, pl.ds(2 * q, 2)],
                                  w_sem.at[slot]).start()

    def start_w2(cb, slot):
        pltpu.make_async_copy(wd_hbm.at[:, :, pl.ds(pl.multiple_of(cb * CB, CB), CB)], ring.at[slot], w_sem.at[slot]).start()

    def wait_w(slot):
        pltpu.make_async_copy(ring.at[slot], ring.at[slot], w_sem.at[slot]).wait()

    for e in range(NSLOT // 2):
        start_w13(wg_hbm, e, 2 * e)
        start_w13(wu_hbm, e, 2 * e + 1)

    cp_i.wait()
    cp_g.wait()
    ids_f = ids_v[...].astype(F32)
    gates_f = gates_v[...]
    meta[0, 0, 0:8, :] = jnp.concatenate([ids_f, ids_f], axis=1)
    meta[0, 0, 8:16, :] = jnp.concatenate([gates_f, gates_f], axis=1)
    cp_x.wait()
    pl.semaphore_wait(barrier, len(PEERS))

    def rows(c, s, h):
        return xs.at[c, pl.ds(s * TOK + h * (TOK // 2), TOK // 2)]

    sends = []

    def send_rows(src, dst, ssem, c, s):
        cp = remote(rows(*src), rows(*dst), ssem, xrecv.at[dst[0], dst[1], dst[2]], c, s)
        cp.start()
        sends.append(cp)

    def wait_rows(c, s, h):
        remote(rows(c, s, h), rows(c, s, h), fsend.at[0], xrecv.at[c, s, h], 0, 1).wait_recv()

    meta_sends = []
    for i, (c, s) in enumerate(PEERS):
        cp = remote(meta.at[0, 0], meta.at[c, s], msend.at[i], mrecv.at[c, s], c, s)
        cp.start()
        meta_sends.append(cp)
    send_rows((0, 0, 1), (1, 0, 1), xsend.at[0], 1, 0)
    send_rows((0, 0, 0), (2, 0, 0), xsend.at[1], 2, 0)
    send_rows((0, 0, 0), (1, 0, 0), xsend.at[2], 1, 0)
    send_rows((0, 0, 1), (2, 0, 1), xsend.at[3], 2, 0)
    send_rows((0, 0, 0), (0, 1, 0), xsend.at[4], 0, 1)
    send_rows((0, 0, 1), (0, 1, 1), xsend.at[5], 0, 1)

    for c, s in PEERS:
        remote(meta.at[c, s], meta.at[c, s], msend.at[0], mrecv.at[c, s], 0, 1).wait_recv()
    base = ((ex * 2 + ey) * 2 + ez) * NEXP
    sub8 = lax.broadcasted_iota(jnp.int32, (NEXP, 128), 0)
    lane8 = lax.broadcasted_iota(jnp.int32, (NEXP, 128), 1)
    mine = (sub8 + base).astype(F32)
    masks, gates = [], []
    for c in range(4):
        m = jnp.where(lane8[0:1] < TOK, meta[c, 0], meta[c, 1])
        mask = jnp.zeros((NEXP, 128), F32)
        gate = jnp.zeros((NEXP, 128), F32)
        for j in range(8):
            hit = m[j:j + 1, :] == mine
            mask += jnp.where(hit, 1.0, 0.0)
            gate += jnp.where(hit, m[8 + j:9 + j, :], 0.0)
        masks.append(mask)
        gates.append(gate)
    r_i = lax.broadcasted_iota(jnp.int32, (128, 128), 0)
    c_i = lax.broadcasted_iota(jnp.int32, (128, 128), 1)
    before = jnp.where((r_i < c_i) & ((r_i < TOK) == (c_i < TOK)), 1.0, 0.0).astype(BF16)
    rank = jnp.dot(jnp.concatenate(masks, axis=0).astype(BF16), before, preferred_element_type=F32)
    sub32 = lax.broadcasted_iota(jnp.int32, (2 * CAP, 128), 0).astype(F32)
    core_off = jnp.where(lane8 < TOK, 0.0, float(CAP))
    for c in range(4):
        code = jnp.where(masks[c] > 0.5, rank[c * NEXP:(c + 1) * NEXP] + core_off, -1.0)
        for e in range(NEXP):
            hit = sub32 == code[e:e + 1, :]
            pmat[c, 2 * CAP * e:2 * CAP * (e + 1), :] = jnp.where(hit, 1.0, 0.0).astype(BF16)
            gtmp[c, 2 * CAP * e:2 * CAP * (e + 1), :] = jnp.where(hit, gates[c][e:e + 1, :], 0.0)
    for c in range(4):
        gt = gtmp[c].T
        hi = gt.astype(BF16)
        rest = gt - hi.astype(F32)
        mid = rest.astype(BF16)
        gmat[c, 0:128, :] = hi
        gmat[c, 128:256, :] = mid
        gmat[c, 256:384, :] = (rest - mid.astype(F32)).astype(BF16)

    def gather(c):
        for nb in range(HID // 512):
            cols = slice(nb * 512, (nb + 1) * 512)
            blk = jnp.dot(pmat[c], xs[c, :, cols], preferred_element_type=F32).astype(BF16)
            for e in range(NEXP):
                xe[e, 2 * CAP * c:2 * CAP * (c + 1), cols] = blk[2 * CAP * e:2 * CAP * (e + 1)]

    wait_rows(1, 0, 1)
    send_rows((1, 0, 1), (3, 0, 1), fsend.at[0], 2, 0)
    send_rows((1, 0, 1), (1, 1, 1), fsend.at[1], 0, 1)
    wait_rows(2, 0, 0)
    send_rows((2, 0, 0), (3, 0, 0), fsend.at[2], 1, 0)
    send_rows((2, 0, 0), (2, 1, 0), fsend.at[3], 0, 1)
    wait_rows(0, 1, 0)
    wait_rows(0, 1, 1)
    gather(0)
    wait_rows(1, 0, 0)
    send_rows((1, 0, 0), (1, 1, 0), fsend.at[4], 0, 1)
    wait_rows(2, 0, 1)
    send_rows((2, 0, 1), (2, 1, 1), fsend.at[5], 0, 1)
    wait_rows(1, 1, 0)
    wait_rows(1, 1, 1)
    gather(1)
    wait_rows(2, 1, 0)
    wait_rows(2, 1, 1)
    gather(2)
    wait_rows(3, 0, 0)
    send_rows((3, 0, 0), (3, 1, 0), fsend.at[6], 0, 1)
    wait_rows(3, 0, 1)
    send_rows((3, 0, 1), (3, 1, 1), fsend.at[7], 0, 1)
    wait_rows(3, 1, 0)
    wait_rows(3, 1, 1)
    gather(3)

    def up(e, carry):
        s1 = lax.rem(2 * e, NSLOT)
        s3 = lax.rem(2 * e + 1, NSLOT)
        wait_w(s1)
        wait_w(s3)
        for q in range(4):
            xin = xe[e]
            h1 = jnp.dot(xin, ring[s1, 2 * q:2 * q + 2].reshape(HID, CB), preferred_element_type=F32)
            h3 = jnp.dot(xin, ring[s3, 2 * q:2 * q + 2].reshape(HID, CB), preferred_element_type=F32)
            act[e, :, q * CB:(q + 1) * CB] = (jax.nn.silu(h1) * h3).astype(BF16)

        @pl.when(e < NEXP - NSLOT // 2)
        def _():
            start_w13(wg_hbm, e + NSLOT // 2, s1)
            start_w13(wu_hbm, e + NSLOT // 2, s3)

        @pl.when((e >= NEXP - NSLOT // 2) & (e < NEXP - 1))
        def _():
            cb = 2 * (e - (NEXP - NSLOT // 2))
            start_w2(cb, s1)
            start_w2(cb + 1, s3)

        return carry

    lax.fori_loop(0, NEXP, up, 0)

    def part(cb):
        slot = lax.rem(N13 + cb, NSLOT)
        wait_w(slot)
        for e in range(NEXP):
            o = jnp.dot(act[e], ring[slot, e], preferred_element_type=F32).astype(BF16)
            for c in range(4):
                obuf[c, 2 * CAP * e:2 * CAP * (e + 1), :] = o[2 * CAP * c:2 * CAP * (c + 1)]
        for c in range(4):
            t = jnp.dot(gmat[c], obuf[c], preferred_element_type=F32)
            t = t[0:128] + t[128:256] + t[256:384]
            acc[cb, c] = t[0:TOK]
            dsend[cb, c] = t[TOK:2 * TOK]
        remote(dsend.at[cb], drecv.at[cb], d_send.at[cb], d_recv.at[cb], 0, 1).start()

    def first(odd):
        return (2, 1) if odd else (1, 2)

    def s2_copies(cb, odd):
        a, b = first(odd)
        return [remote(acc.at[cb, a], r2.at[cb, 0], s2_send.at[cb, 0], s2_recv.at[cb, 0], a, 0),
                remote(acc.at[cb, 3], r2.at[cb, 1], s2_send.at[cb, 1], s2_recv.at[cb, 1], a, 0)]

    def stage2(cb, odd):
        remote(dsend.at[cb], drecv.at[cb], d_send.at[cb], d_recv.at[cb], 0, 1).wait_recv()
        acc[cb] = acc[cb] + drecv[cb]
        cps = s2_copies(cb, odd)
        cps[1].start()
        cps[0].start()

    def s3_copy(cb, odd):
        a, b = first(odd)
        return remote(f3.at[cb], r3.at[cb], s3_send.at[cb], s3_recv.at[cb], b, 0)

    def stage3(cb, odd):
        a, b = first(odd)
        s2_copies(cb, odd)[1].wait_recv()
        f3[cb] = acc[cb, b] + r2[cb, 1]
        s3_copy(cb, odd).start()

    def y_copy(cb):
        cols = pl.ds(pl.multiple_of(cb * CB, CB), CB)
        return pltpu.make_async_copy(yv.at[cb], y_hbm.at[:, cols], y_sem.at[cb])

    def final(cb, odd):
        s2_copies(cb, odd)[0].wait_recv()
        s3_copy(cb, odd).wait_recv()
        cols = pl.ds(pl.multiple_of(cb * CB, CB), CB)
        xin = xs[0, 0:TOK, cols].astype(F32)
        yv[cb] = (xin + ((acc[cb, 0] + r2[cb, 0]) + r3[cb])).astype(BF16)
        y_copy(cb).start()

    def down(i, carry):
        part(2 * i)

        @pl.when(i > 0)
        def _():
            stage2(2 * i - 1, 1)

        part(2 * i + 1)
        stage2(2 * i, 0)
        return carry

    lax.fori_loop(0, NCB // 2, down, 0)
    stage2(NCB - 1, 1)

    def third(i, carry):
        stage3(2 * i, 0)
        stage3(2 * i + 1, 1)
        return carry

    lax.fori_loop(0, NCB // 2, third, 0)

    def last(i, carry):
        final(2 * i, 0)
        final(2 * i + 1, 1)
        return carry

    lax.fori_loop(0, NCB // 2, last, 0)

    for cp in sends + meta_sends:
        cp.wait_send()
    for cb in range(NCB):
        remote(dsend.at[cb], drecv.at[cb], d_send.at[cb], d_recv.at[cb], 0, 1).wait_send()
        for cp in s2_copies(cb, cb & 1):
            cp.wait_send()
        s3_copy(cb, cb & 1).wait_send()
        y_copy(cb).wait()


def solution(mesh):
    def local_layer(x_loc, ids_loc, gates_loc, w_g, w_u, w_d):
        w_g = w_g.reshape(NEXP, 2, FFN, FFN)
        w_u = w_u.reshape(NEXP, 2, FFN, FFN)
        any_spec = pl.BlockSpec(memory_space=pl.ANY)
        dma = pltpu.SemaphoreType.DMA
        return pl.pallas_call(
            kernel,
            out_shape=jax.ShapeDtypeStruct((TOK, HID), BF16),
            in_specs=[any_spec] * 6,
            out_specs=any_spec,
            scratch_shapes=[
                pltpu.VMEM((NSLOT, NEXP, FFN, CB), BF16),
                pltpu.VMEM((4, 2 * TOK, HID), BF16),
                pltpu.VMEM((NEXP, 8 * CAP, HID), BF16),
                pltpu.VMEM((NEXP, 8 * CAP, FFN), BF16),
                pltpu.VMEM((NCB, 4, TOK, CB), F32),
                pltpu.VMEM((NCB, 4, TOK, CB), F32),
                pltpu.VMEM((NCB, 4, TOK, CB), F32),
                pltpu.VMEM((NCB, 2, TOK, CB), F32),
                pltpu.VMEM((NCB, TOK, CB), F32),
                pltpu.VMEM((NCB, TOK, CB), F32),
                pltpu.VMEM((4, 2 * CAP * NEXP, 128), BF16),
                pltpu.VMEM((4, 2 * CAP * NEXP, 128), F32),
                pltpu.VMEM((4, 384, 2 * CAP * NEXP), BF16),
                pltpu.VMEM((4, 2 * CAP * NEXP, CB), BF16),
                pltpu.VMEM((8, TOK), jnp.int32),
                pltpu.VMEM((8, TOK), F32),
                pltpu.VMEM((4, 2, 16, 128), F32),
                pltpu.VMEM((NCB, TOK, CB), BF16),
                dma((NSLOT,)),
                dma((3,)),
                dma((6,)),
                dma((4, 2, 2)),
                dma((8,)),
                dma((7,)),
                dma((4, 2)),
                dma((NCB,)),
                dma((NCB,)),
                dma((NCB, 2)),
                dma((NCB, 2)),
                dma((NCB,)),
                dma((NCB,)),
                dma((NCB,)),
            ],
            compiler_params=pltpu.CompilerParams(collective_id=0, has_side_effects=True,
                                                 vmem_limit_bytes=67043328),
            name='moe_decode',
        )(x_loc, ids_loc.T, gates_loc.T, w_g, w_u, w_d)

    tok_spec = P(TOKEN_AXES, None)
    w_spec = P(EXPERT_AXES, None, None)
    return jax.shard_map(local_layer, mesh=mesh, in_specs=(tok_spec, tok_spec, tok_spec, w_spec, w_spec, w_spec), out_specs=tok_spec, check_vma=False)
```

```python
import jax
import jax.numpy as jnp
from jax import lax
from jax.experimental import pallas as pl
from jax.experimental.pallas import tpu as pltpu
from jax.sharding import PartitionSpec as P

TOKEN_AXES = ('ez', 'ey', 'ex')
EXPERT_AXES = ('ex', 'ey', 'ez')
MESH = pl.DeviceIdType.MESH
F32 = jnp.float32
BF16 = jnp.bfloat16

TOK = 64
HALF = TOK // 2
HID = 2048
FFN = 1024
NEXP = 8
CAP = 16
NSLOT = 9
CB = 256
NCB = HID // CB
N13 = 2 * NEXP

PEERS = [(c, s) for c in range(4) for s in range(2) if (c, s) != (0, 0)]
STAY = ((0, 2), (0, 1))
LEAVE = ((1, 3), (2, 3))
HOP1 = (1, 2)
HOP2 = (2, 1)


def kernel(x_hbm, ids_hbm, gates_hbm, wg_hbm, wu_hbm, wd_hbm, y_ref,
           ring, xs, xe, hbuf, act, drecv, r2, r3, pmat, gtmp, gmat, obuf, ids_v, gates_v, meta,
           w_sem, loc_sem, xsend, xrecv, msend, mrecv, d_send, d_recv, s2_send, s2_recv, s3_send, s3_recv):
    ez, ey, ex = lax.axis_index('ez'), lax.axis_index('ey'), lax.axis_index('ex')

    def dev(c, s):
        return (1 - ez if c & 2 else ez, 1 - ey if c & 1 else ey, 1 - ex if s else ex)

    def remote(src, dst, ssem, rsem, c, s):
        return pltpu.make_async_remote_copy(src_ref=src, dst_ref=dst, send_sem=ssem, recv_sem=rsem,
                                            device_id=dev(c, s), device_id_type=MESH)

    cp_x = [pltpu.make_async_copy(x_hbm.at[:, pl.ds(k * FFN, FFN)], xs.at[k, 0, pl.ds(0, TOK)], loc_sem.at[k])
            for k in range(2)]
    cp_i = pltpu.make_async_copy(ids_hbm, ids_v, loc_sem.at[2])
    cp_g = pltpu.make_async_copy(gates_hbm, gates_v, loc_sem.at[3])
    for cp in (cp_x[0], cp_i, cp_g, cp_x[1]):
        cp.start()

    barrier = pltpu.get_barrier_semaphore()
    for c, s in PEERS:
        pl.semaphore_signal(barrier, inc=1, device_id=dev(c, s), device_id_type=MESH)

    def start_w13(k, e, slot):
        for i, w_hbm in enumerate((wg_hbm, wu_hbm)):
            for q in range(4):
                pltpu.make_async_copy(w_hbm.at[e, k, :, pl.ds(q * CB, CB)], ring.at[slot, 4 * i + q],
                                      w_sem.at[slot]).start()

    def start_w2(cb, slot):
        pltpu.make_async_copy(wd_hbm.at[:, :, pl.ds(pl.multiple_of(cb * CB, CB), CB)], ring.at[slot],
                              w_sem.at[slot]).start()

    def wait_w(slot):
        pltpu.make_async_copy(ring.at[slot], ring.at[slot], w_sem.at[slot]).wait()

    for u in range(NSLOT):
        start_w13(u // NEXP, u % NEXP, u)

    cp_i.wait()
    cp_g.wait()
    ids_f = ids_v[...].astype(F32)
    gates_f = gates_v[...]
    meta[0, 0, 0:8, :] = jnp.concatenate([ids_f, ids_f], axis=1)
    meta[0, 0, 8:16, :] = jnp.concatenate([gates_f, gates_f], axis=1)
    cp_x[0].wait()
    cp_x[1].wait()
    pl.semaphore_wait(barrier, len(PEERS))

    def rows(k, c, s, h):
        return xs.at[k, c, pl.ds(s * TOK + h * HALF, HALF)]

    def row_copy(k, src, dst, c, s):
        return remote(rows(k, *src), rows(k, *dst), xsend.at[k, dst[0], dst[1], dst[2]],
                      xrecv.at[k, dst[0], dst[1], dst[2]], c, s)

    ROUTES = {}
    for c in (1, 2):
        for h in range(2):
            ROUTES[(c, 0, h)] = ((0, 0, h), c, 0)
    ROUTES[(3, 0, 1)] = ((1, 0, 1), 2, 0)
    ROUTES[(3, 0, 0)] = ((2, 0, 0), 1, 0)
    for c in range(4):
        for h in range(2):
            ROUTES[(c, 1, h)] = ((c, 0, h), 0, 1)

    def send_rows(k, *dst):
        src, c, s = ROUTES[dst]
        row_copy(k, src, dst, c, s).start()

    def wait_rows(k, *dst):
        src, c, s = ROUTES[dst]
        row_copy(k, src, dst, c, s).wait_recv()

    def send_own(k):
        send_rows(k, 1, 0, 1)
        send_rows(k, 2, 0, 0)
        send_rows(k, 1, 0, 0)
        send_rows(k, 2, 0, 1)
        send_rows(k, 0, 1, 0)
        send_rows(k, 0, 1, 1)

    def forward_first(k):
        wait_rows(k, 1, 0, 1)
        send_rows(k, 3, 0, 1)
        send_rows(k, 1, 1, 1)
        wait_rows(k, 2, 0, 0)
        send_rows(k, 3, 0, 0)
        send_rows(k, 2, 1, 0)

    def forward_second(k):
        wait_rows(k, 1, 0, 0)
        send_rows(k, 1, 1, 0)
        wait_rows(k, 2, 0, 1)
        send_rows(k, 2, 1, 1)

    def forward_third(k):
        for h in range(2):
            wait_rows(k, 3, 0, h)
            send_rows(k, 3, 1, h)

    meta_sends = []
    for i, (c, s) in enumerate(PEERS):
        cp = remote(meta.at[0, 0], meta.at[c, s], msend.at[i], mrecv.at[c, s], c, s)
        cp.start()
        meta_sends.append(cp)
    send_own(0)
    forward_first(0)
    send_own(1)

    for c, s in PEERS:
        remote(meta.at[c, s], meta.at[c, s], msend.at[0], mrecv.at[c, s], 0, 1).wait_recv()
    base = ((ex * 2 + ey) * 2 + ez) * NEXP
    sub8 = lax.broadcasted_iota(jnp.int32, (NEXP, 128), 0)
    lane8 = lax.broadcasted_iota(jnp.int32, (NEXP, 128), 1)
    mine = (sub8 + base).astype(F32)
    masks, gates = [], []
    for c in range(4):
        m = jnp.where(lane8[0:1] < TOK, meta[c, 0], meta[c, 1])
        mask = jnp.zeros((NEXP, 128), F32)
        gate = jnp.zeros((NEXP, 128), F32)
        for j in range(8):
            hit = m[j:j + 1, :] == mine
            mask += jnp.where(hit, 1.0, 0.0)
            gate += jnp.where(hit, m[8 + j:9 + j, :], 0.0)
        masks.append(mask)
        gates.append(gate)
    r_i = lax.broadcasted_iota(jnp.int32, (128, 128), 0)
    c_i = lax.broadcasted_iota(jnp.int32, (128, 128), 1)
    before = jnp.where((r_i < c_i) & ((r_i < TOK) == (c_i < TOK)), 1.0, 0.0).astype(BF16)
    rank = jnp.dot(jnp.concatenate(masks, axis=0).astype(BF16), before, preferred_element_type=F32)
    sub32 = lax.broadcasted_iota(jnp.int32, (2 * CAP, 128), 0).astype(F32)
    core_off = jnp.where(lane8 < TOK, 0.0, float(CAP))
    for c in range(4):
        code = jnp.where(masks[c] > 0.5, rank[c * NEXP:(c + 1) * NEXP] + core_off, -1.0)
        for e in range(NEXP):
            hit = sub32 == code[e:e + 1, :]
            pmat[c, 2 * CAP * e:2 * CAP * (e + 1), :] = jnp.where(hit, 1.0, 0.0).astype(BF16)
            gtmp[c, 2 * CAP * e:2 * CAP * (e + 1), :] = jnp.where(hit, gates[c][e:e + 1, :], 0.0)
    for c in range(4):
        gt = gtmp[c].T
        hi = gt.astype(BF16)
        rest = gt - hi.astype(F32)
        mid = rest.astype(BF16)
        gmat[c, 0:128, :] = hi
        gmat[c, 128:256, :] = mid
        gmat[c, 256:384, :] = (rest - mid.astype(F32)).astype(BF16)

    def gather(k, c):
        for h in range(2):
            if (c, 1, h) in ROUTES:
                wait_rows(k, c, 1, h)
        for nb in range(FFN // 512):
            cols = slice(nb * 512, (nb + 1) * 512)
            blk = jnp.dot(pmat[c], xs[k, c, :, cols], preferred_element_type=F32).astype(BF16)
            for e in range(NEXP):
                xe[k, e, 2 * CAP * c:2 * CAP * (c + 1), cols] = blk[2 * CAP * e:2 * CAP * (e + 1)]

    gather(0, 0)
    forward_second(0)
    gather(0, 1)
    gather(0, 2)
    forward_third(0)
    gather(0, 3)

    def refill(u, slot):
        nxt = u + NSLOT

        @pl.when(nxt < N13)
        def _():
            start_w13(nxt // NEXP, lax.rem(nxt, NEXP), slot)

        @pl.when((nxt >= N13) & (nxt < N13 + NCB))
        def _():
            start_w2(nxt - N13, slot)

    def up0(e, carry):
        slot = lax.rem(e, NSLOT)
        wait_w(slot)
        for q in range(8):
            hbuf[e, q] = jnp.dot(xe[0, e], ring[slot, q], preferred_element_type=F32)
        refill(e, slot)

        @pl.when(e == 0)
        def _():
            forward_first(1)

        @pl.when(e == 2)
        def _():
            forward_second(1)
            gather(1, 0)

        @pl.when(e == 5)
        def _():
            gather(1, 1)
            gather(1, 2)
            forward_third(1)

        return carry

    lax.fori_loop(0, NEXP, up0, 0)
    gather(1, 3)

    def up1(e, carry):
        u = e + NEXP
        slot = lax.rem(u, NSLOT)
        wait_w(slot)
        for q in range(4):
            h1 = hbuf[e, q] + jnp.dot(xe[1, e], ring[slot, q], preferred_element_type=F32)
            h3 = hbuf[e, 4 + q] + jnp.dot(xe[1, e], ring[slot, 4 + q], preferred_element_type=F32)
            act[e, :, q * CB:(q + 1) * CB] = (jax.nn.silu(h1) * h3).astype(BF16)
        refill(u, slot)
        return carry

    lax.fori_loop(0, NEXP, up1, 0)

    def d_copy(cb, g):
        return remote(hbuf.at[cb, g], drecv.at[cb, g], d_send.at[cb, g], d_recv.at[cb, g], 0, 1)

    def s2_copy(cb, h):
        return remote(hbuf.at[cb, 3, pl.ds(h * TOK, TOK)], r2.at[cb, pl.ds(h * TOK, TOK)],
                      s2_send.at[cb, h], s2_recv.at[cb, h], HOP1[h], 0)

    def s3_copy(cb, h):
        return remote(hbuf.at[cb, 2, pl.ds(h * TOK + HALF, HALF)], r3.at[cb, pl.ds(h * HALF, HALF)],
                      s3_send.at[cb, h], s3_recv.at[cb, h], HOP2[h], 0)

    def part(cb):
        slot = lax.rem(N13 + cb, NSLOT)
        wait_w(slot)
        for e in range(NEXP):
            o = jnp.dot(act[e], ring[slot, e], preferred_element_type=F32).astype(BF16)
            for c in range(4):
                obuf[c, 2 * CAP * e:2 * CAP * (e + 1), :] = o[2 * CAP * c:2 * CAP * (c + 1)]
        for c in (3, 1, 2, 0):
            t = jnp.dot(gmat[c], obuf[c], preferred_element_type=F32)
            t = t[0:128] + t[128:256] + t[256:384]
            for h in range(2):
                g = 0 if c in STAY[h] else 1
                place = (LEAVE if g else STAY)[h].index(c)
                at = pl.ds(h * TOK + place * HALF, HALF)
                hbuf[cb, 2 + g, at] = t[h * HALF:(h + 1) * HALF]
                hbuf[cb, g, at] = t[TOK + h * HALF:TOK + (h + 1) * HALF]
        d_copy(cb, 1).start()
        d_copy(cb, 0).start()

    def stage2(cb):
        d_copy(cb, 1).wait_recv()
        hbuf[cb, 3] = hbuf[cb, 3] + drecv[cb, 1]
        s2_copy(cb, 0).start()
        s2_copy(cb, 1).start()

    def down(cb, carry):
        part(cb)

        @pl.when(cb > 0)
        def _():
            stage2(cb - 1)

        return carry

    lax.fori_loop(0, NCB, down, 0)
    stage2(NCB - 1)

    def third(cb, carry):
        d_copy(cb, 0).wait_recv()
        for h in range(2):
            s2_copy(cb, h).wait_recv()
        hbuf[cb, 2] = (hbuf[cb, 2] + drecv[cb, 0]) + r2[cb]
        for h in range(2):
            s3_copy(cb, h).start()
        return carry

    lax.fori_loop(0, NCB, third, 0)

    def last(cb, carry):
        cols = pl.ds(pl.multiple_of(lax.rem(cb, 4) * CB, CB), CB)
        ycols = pl.ds(pl.multiple_of(cb * CB, CB), CB)
        for h in range(2):
            s3_copy(cb, h).wait_recv()
            at = pl.ds(h * HALF, HALF)
            xin = xs[cb // 4, 0, at, cols].astype(F32)
            y_ref[at, ycols] = (xin + (hbuf[cb, 2, pl.ds(h * TOK, HALF)] + r3[cb, at])).astype(BF16)
        return carry

    lax.fori_loop(0, NCB, last, 0)

    for cp in meta_sends:
        cp.wait_send()
    for k in range(2):
        for dst, (src, c, s) in ROUTES.items():
            row_copy(k, src, dst, c, s).wait_send()
    for cb in range(NCB):
        for i in range(2):
            d_copy(cb, i).wait_send()
            s2_copy(cb, i).wait_send()
            s3_copy(cb, i).wait_send()


def solution(mesh):
    def local_layer(x_loc, ids_loc, gates_loc, w_g, w_u, w_d):
        w_g = w_g.reshape(NEXP, 2, FFN, FFN)
        w_u = w_u.reshape(NEXP, 2, FFN, FFN)
        any_spec = pl.BlockSpec(memory_space=pl.ANY)
        dma = pltpu.SemaphoreType.DMA
        return pl.pallas_call(
            kernel,
            out_shape=jax.ShapeDtypeStruct((TOK, HID), BF16),
            in_specs=[any_spec] * 6,
            out_specs=pl.BlockSpec(memory_space=pltpu.VMEM),
            scratch_shapes=[
                pltpu.VMEM((NSLOT, NEXP, FFN, CB), BF16),
                pltpu.VMEM((2, 4, 2 * TOK, FFN), BF16),
                pltpu.VMEM((2, NEXP, 8 * CAP, FFN), BF16),
                pltpu.VMEM((NEXP, 8, 8 * CAP, CB), F32),
                pltpu.VMEM((NEXP, 8 * CAP, FFN), BF16),
                pltpu.VMEM((NCB, 2, 2 * TOK, CB), F32),
                pltpu.VMEM((NCB, 2 * TOK, CB), F32),
                pltpu.VMEM((NCB, TOK, CB), F32),
                pltpu.VMEM((4, 2 * CAP * NEXP, 128), BF16),
                pltpu.VMEM((4, 2 * CAP * NEXP, 128), F32),
                pltpu.VMEM((4, 384, 2 * CAP * NEXP), BF16),
                pltpu.VMEM((4, 2 * CAP * NEXP, CB), BF16),
                pltpu.VMEM((8, TOK), jnp.int32),
                pltpu.VMEM((8, TOK), F32),
                pltpu.VMEM((4, 2, 16, 128), F32),
                dma((NSLOT,)),
                dma((4,)),
                dma((2, 4, 2, 2)),
                dma((2, 4, 2, 2)),
                dma((7,)),
                dma((4, 2)),
                dma((NCB, 2)),
                dma((NCB, 2)),
                dma((NCB, 2)),
                dma((NCB, 2)),
                dma((NCB, 2)),
                dma((NCB, 2)),
            ],
            compiler_params=pltpu.CompilerParams(collective_id=0, has_side_effects=True,
                                                 vmem_limit_bytes=67043328),
            name='moe_decode',
        )(x_loc, ids_loc.T, gates_loc.T, w_g, w_u, w_d)

    tok_spec = P(TOKEN_AXES, None)
    w_spec = P(EXPERT_AXES, None, None)
    return jax.shard_map(local_layer, mesh=mesh, in_specs=(tok_spec, tok_spec, tok_spec, w_spec, w_spec, w_spec), out_specs=tok_spec, check_vma=False)
```

```python
import jax
import jax.numpy as jnp
from jax import lax
from jax.experimental import pallas as pl
from jax.experimental.pallas import tpu as pltpu
from jax.sharding import PartitionSpec as P

TOKEN_AXES = ('ez', 'ey', 'ex')
EXPERT_AXES = ('ex', 'ey', 'ez')
MESH = pl.DeviceIdType.MESH
F32 = jnp.float32
BF16 = jnp.bfloat16

TOK = 64
HALF = TOK // 2
HID = 2048
FFN = 1024
NEXP = 8
CAP = 16
NSLOT = 9
CB = 256
NCB = HID // CB
N13 = 2 * NEXP

PEERS = [(c, s) for c in range(4) for s in range(2) if (c, s) != (0, 0)]
STAY = ((0, 2), (0, 1))
LEAVE = ((1, 3), (2, 3))
HOP1 = (1, 2)
HOP2 = (2, 1)


def kernel(x_hbm, ids_hbm, gates_hbm, wg_hbm, wu_hbm, wd_hbm, y_ref,
           ring, xs, xe, hbuf, act, drecv, r2, r3, pmat, gtmp, gmat, obuf, ids_v, gates_v, meta,
           w_sem, loc_sem, xsend, xrecv, msend, mrecv, d_send, d_recv, s2_send, s2_recv, s3_send, s3_recv):
    ez, ey, ex = lax.axis_index('ez'), lax.axis_index('ey'), lax.axis_index('ex')

    def dev(c, s):
        return (1 - ez if c & 2 else ez, 1 - ey if c & 1 else ey, 1 - ex if s else ex)

    def remote(src, dst, ssem, rsem, c, s):
        return pltpu.make_async_remote_copy(src_ref=src, dst_ref=dst, send_sem=ssem, recv_sem=rsem,
                                            device_id=dev(c, s), device_id_type=MESH)

    cp_x = [pltpu.make_async_copy(x_hbm.at[:, pl.ds(k * FFN, FFN)], xs.at[k, 0, pl.ds(0, TOK)], loc_sem.at[k])
            for k in range(2)]
    cp_i = pltpu.make_async_copy(ids_hbm, ids_v, loc_sem.at[2])
    cp_g = pltpu.make_async_copy(gates_hbm, gates_v, loc_sem.at[3])
    for cp in (cp_x[0], cp_i, cp_g, cp_x[1]):
        cp.start()

    barrier = pltpu.get_barrier_semaphore()
    for c, s in PEERS:
        pl.semaphore_signal(barrier, inc=1, device_id=dev(c, s), device_id_type=MESH)

    def start_w13(k, e, slot):
        for i, w_hbm in enumerate((wg_hbm, wu_hbm)):
            pltpu.make_async_copy(w_hbm.at[e, k], ring.at[slot, i], w_sem.at[slot]).start()

    def start_w2(cb, slot):
        cols = pl.ds(pl.multiple_of(cb * CB, CB), CB)
        for e in range(NEXP):
            pltpu.make_async_copy(wd_hbm.at[e, :, cols], ring.at[slot, e // 4, :, pl.ds(e % 4 * CB, CB)],
                                  w_sem.at[slot]).start()

    def wait_w(slot):
        pltpu.make_async_copy(ring.at[slot], ring.at[slot], w_sem.at[slot]).wait()

    def wcols(slot, i):
        return ring[slot, i // 4, :, i % 4 * CB:(i % 4 + 1) * CB]

    for u in range(NSLOT):
        start_w13(u // NEXP, u % NEXP, u)

    cp_i.wait()
    cp_g.wait()
    ids_f = ids_v[...].astype(F32)
    gates_f = gates_v[...]
    meta[0, 0, 0:8, :] = jnp.concatenate([ids_f, ids_f], axis=1)
    meta[0, 0, 8:16, :] = jnp.concatenate([gates_f, gates_f], axis=1)
    cp_x[0].wait()
    cp_x[1].wait()
    pl.semaphore_wait(barrier, len(PEERS))

    def rows(k, c, s, h):
        return xs.at[k, c, pl.ds(s * TOK + h * HALF, HALF)]

    def row_copy(k, src, dst, c, s):
        return remote(rows(k, *src), rows(k, *dst), xsend.at[k, dst[0], dst[1], dst[2]],
                      xrecv.at[k, dst[0], dst[1], dst[2]], c, s)

    ROUTES = {}
    for c in (1, 2):
        for h in range(2):
            ROUTES[(c, 0, h)] = ((0, 0, h), c, 0)
    ROUTES[(3, 0, 1)] = ((1, 0, 1), 2, 0)
    ROUTES[(3, 0, 0)] = ((2, 0, 0), 1, 0)
    for c in range(4):
        for h in range(2):
            ROUTES[(c, 1, h)] = ((c, 0, h), 0, 1)

    def send_rows(k, *dst):
        src, c, s = ROUTES[dst]
        row_copy(k, src, dst, c, s).start()

    def wait_rows(k, *dst):
        src, c, s = ROUTES[dst]
        row_copy(k, src, dst, c, s).wait_recv()

    def send_first(k):
        send_rows(k, 1, 0, 1)
        send_rows(k, 2, 0, 0)

    def send_second(k):
        send_rows(k, 1, 0, 0)
        send_rows(k, 2, 0, 1)
        send_rows(k, 0, 1, 0)
        send_rows(k, 0, 1, 1)

    def forward_first(k):
        wait_rows(k, 1, 0, 1)
        send_rows(k, 3, 0, 1)
        send_rows(k, 1, 1, 1)
        wait_rows(k, 2, 0, 0)
        send_rows(k, 3, 0, 0)
        send_rows(k, 2, 1, 0)

    def forward_second(k):
        wait_rows(k, 1, 0, 0)
        send_rows(k, 1, 1, 0)
        wait_rows(k, 2, 0, 1)
        send_rows(k, 2, 1, 1)

    def forward_third(k):
        for h in range(2):
            wait_rows(k, 3, 0, h)
            send_rows(k, 3, 1, h)

    meta_sends = []
    for i, (c, s) in enumerate(PEERS):
        cp = remote(meta.at[0, 0], meta.at[c, s], msend.at[i], mrecv.at[c, s], c, s)
        cp.start()
        meta_sends.append(cp)
    send_first(0)
    send_second(0)
    send_first(1)
    forward_first(0)
    send_second(1)

    for c, s in PEERS:
        remote(meta.at[c, s], meta.at[c, s], msend.at[0], mrecv.at[c, s], 0, 1).wait_recv()
    base = ((ex * 2 + ey) * 2 + ez) * NEXP
    sub8 = lax.broadcasted_iota(jnp.int32, (NEXP, 128), 0)
    lane8 = lax.broadcasted_iota(jnp.int32, (NEXP, 128), 1)
    mine = (sub8 + base).astype(F32)
    masks, gates = [], []
    for c in range(4):
        m = jnp.where(lane8[0:1] < TOK, meta[c, 0], meta[c, 1])
        mask = jnp.zeros((NEXP, 128), F32)
        gate = jnp.zeros((NEXP, 128), F32)
        for j in range(8):
            hit = m[j:j + 1, :] == mine
            mask += jnp.where(hit, 1.0, 0.0)
            gate += jnp.where(hit, m[8 + j:9 + j, :], 0.0)
        masks.append(mask)
        gates.append(gate)
    r_i = lax.broadcasted_iota(jnp.int32, (128, 128), 0)
    c_i = lax.broadcasted_iota(jnp.int32, (128, 128), 1)
    before = jnp.where((r_i < c_i) & ((r_i < TOK) == (c_i < TOK)), 1.0, 0.0).astype(BF16)
    rank = jnp.dot(jnp.concatenate(masks, axis=0).astype(BF16), before, preferred_element_type=F32)
    sub32 = lax.broadcasted_iota(jnp.int32, (2 * CAP, 128), 0).astype(F32)
    core_off = jnp.where(lane8 < TOK, 0.0, float(CAP))
    for c in range(4):
        code = jnp.where(masks[c] > 0.5, rank[c * NEXP:(c + 1) * NEXP] + core_off, -1.0)
        for e in range(NEXP):
            hit = sub32 == code[e:e + 1, :]
            pmat[c, 2 * CAP * e:2 * CAP * (e + 1), :] = jnp.where(hit, 1.0, 0.0).astype(BF16)
            gtmp[c, 2 * CAP * e:2 * CAP * (e + 1), :] = jnp.where(hit, gates[c][e:e + 1, :], 0.0)
    for c in range(4):
        gt = gtmp[c].T
        hi = gt.astype(BF16)
        rest = gt - hi.astype(F32)
        mid = rest.astype(BF16)
        gmat[c, 0:128, :] = hi
        gmat[c, 128:256, :] = mid
        gmat[c, 256:384, :] = (rest - mid.astype(F32)).astype(BF16)

    def gather(k, c):
        for h in range(2):
            if (c, 1, h) in ROUTES:
                wait_rows(k, c, 1, h)
        for nb in range(FFN // 512):
            cols = slice(nb * 512, (nb + 1) * 512)
            blk = jnp.dot(pmat[c], xs[k, c, :, cols], preferred_element_type=F32).astype(BF16)
            for e in range(NEXP):
                xe[k, e, 2 * CAP * c:2 * CAP * (c + 1), cols] = blk[2 * CAP * e:2 * CAP * (e + 1)]

    gather(0, 0)
    forward_second(0)
    gather(0, 1)
    gather(0, 2)
    forward_first(1)
    forward_third(0)
    gather(0, 3)

    def refill(u, slot):
        nxt = u + NSLOT

        @pl.when(nxt < N13)
        def _():
            start_w13(nxt // NEXP, lax.rem(nxt, NEXP), slot)

        @pl.when((nxt >= N13) & (nxt < N13 + NCB))
        def _():
            start_w2(nxt - N13, slot)

    def up0(e, carry):
        slot = lax.rem(e, NSLOT)
        wait_w(slot)
        for q in range(8):
            hbuf[e, q] = jnp.dot(xe[0, e], wcols(slot, q), preferred_element_type=F32)
        refill(e, slot)

        @pl.when(e == 0)
        def _():
            forward_second(1)

        @pl.when(e == 2)
        def _():
            forward_third(1)
            gather(1, 0)

        @pl.when(e == 4)
        def _():
            gather(1, 1)
            gather(1, 2)

        return carry

    lax.fori_loop(0, NEXP, up0, 0)
    gather(1, 3)

    def up1(e, carry):
        u = e + NEXP
        slot = lax.rem(u, NSLOT)
        wait_w(slot)
        for q in range(4):
            h1 = hbuf[e, q] + jnp.dot(xe[1, e], wcols(slot, q), preferred_element_type=F32)
            h3 = hbuf[e, 4 + q] + jnp.dot(xe[1, e], wcols(slot, 4 + q), preferred_element_type=F32)
            act[e, :, q * CB:(q + 1) * CB] = (jax.nn.silu(h1) * h3).astype(BF16)
        refill(u, slot)
        return carry

    lax.fori_loop(0, NEXP, up1, 0)

    def d_copy(cb, g):
        return remote(hbuf.at[cb, g], drecv.at[cb, g], d_send.at[cb, g], d_recv.at[cb, g], 0, 1)

    def s2_copy(cb, h):
        return remote(hbuf.at[cb, 3, pl.ds(h * TOK, TOK)], r2.at[cb, pl.ds(h * TOK, TOK)],
                      s2_send.at[cb, h], s2_recv.at[cb, h], HOP1[h], 0)

    def s3_copy(cb, h):
        return remote(hbuf.at[cb, 2, pl.ds(h * TOK + HALF, HALF)], r3.at[cb, pl.ds(h * HALF, HALF)],
                      s3_send.at[cb, h], s3_recv.at[cb, h], HOP2[h], 0)

    def part(cb):
        slot = lax.rem(N13 + cb, NSLOT)
        wait_w(slot)
        for e in range(NEXP):
            o = jnp.dot(act[e], wcols(slot, e), preferred_element_type=F32).astype(BF16)
            for c in range(4):
                obuf[c, 2 * CAP * e:2 * CAP * (e + 1), :] = o[2 * CAP * c:2 * CAP * (c + 1)]
        for c in (3, 1, 2, 0):
            t = jnp.dot(gmat[c], obuf[c], preferred_element_type=F32)
            t = t[0:128] + t[128:256] + t[256:384]
            for h in range(2):
                g = 0 if c in STAY[h] else 1
                place = (LEAVE if g else STAY)[h].index(c)
                at = pl.ds(h * TOK + place * HALF, HALF)
                hbuf[cb, 2 + g, at] = t[h * HALF:(h + 1) * HALF]
                hbuf[cb, g, at] = t[TOK + h * HALF:TOK + (h + 1) * HALF]
        d_copy(cb, 1).start()
        d_copy(cb, 0).start()

    def stage2(cb):
        d_copy(cb, 1).wait_recv()
        hbuf[cb, 3] = hbuf[cb, 3] + drecv[cb, 1]
        s2_copy(cb, 0).start()
        s2_copy(cb, 1).start()

    def down(cb, carry):
        part(cb)

        @pl.when(cb > 0)
        def _():
            stage2(cb - 1)

        return carry

    lax.fori_loop(0, NCB, down, 0)
    stage2(NCB - 1)

    def third(cb, carry):
        d_copy(cb, 0).wait_recv()
        for h in range(2):
            s2_copy(cb, h).wait_recv()
        hbuf[cb, 2] = (hbuf[cb, 2] + drecv[cb, 0]) + r2[cb]
        for h in range(2):
            s3_copy(cb, h).start()
        return carry

    lax.fori_loop(0, NCB, third, 0)

    def last(cb, carry):
        cols = pl.ds(pl.multiple_of(lax.rem(cb, 4) * CB, CB), CB)
        ycols = pl.ds(pl.multiple_of(cb * CB, CB), CB)
        for h in range(2):
            s3_copy(cb, h).wait_recv()
            at = pl.ds(h * HALF, HALF)
            xin = xs[cb // 4, 0, at, cols].astype(F32)
            y_ref[at, ycols] = (xin + (hbuf[cb, 2, pl.ds(h * TOK, HALF)] + r3[cb, at])).astype(BF16)
        return carry

    lax.fori_loop(0, NCB, last, 0)

    for cp in meta_sends:
        cp.wait_send()
    for k in range(2):
        for dst, (src, c, s) in ROUTES.items():
            row_copy(k, src, dst, c, s).wait_send()
    for cb in range(NCB):
        for i in range(2):
            d_copy(cb, i).wait_send()
            s2_copy(cb, i).wait_send()
            s3_copy(cb, i).wait_send()


def solution(mesh):
    def local_layer(x_loc, ids_loc, gates_loc, w_g, w_u, w_d):
        w_g = w_g.reshape(NEXP, 2, FFN, FFN)
        w_u = w_u.reshape(NEXP, 2, FFN, FFN)
        any_spec = pl.BlockSpec(memory_space=pl.ANY)
        dma = pltpu.SemaphoreType.DMA
        return pl.pallas_call(
            kernel,
            out_shape=pltpu.VMEM((TOK, HID), BF16),
            in_specs=[any_spec] * 6,
            out_specs=pl.BlockSpec(memory_space=pltpu.VMEM),
            scratch_shapes=[
                pltpu.VMEM((NSLOT, 2, FFN, FFN), BF16),
                pltpu.VMEM((2, 4, 2 * TOK, FFN), BF16),
                pltpu.VMEM((2, NEXP, 8 * CAP, FFN), BF16),
                pltpu.VMEM((NEXP, 8, 8 * CAP, CB), F32),
                pltpu.VMEM((NEXP, 8 * CAP, FFN), BF16),
                pltpu.VMEM((NCB, 2, 2 * TOK, CB), F32),
                pltpu.VMEM((NCB, 2 * TOK, CB), F32),
                pltpu.VMEM((NCB, TOK, CB), F32),
                pltpu.VMEM((4, 2 * CAP * NEXP, 128), BF16),
                pltpu.VMEM((4, 2 * CAP * NEXP, 128), F32),
                pltpu.VMEM((4, 384, 2 * CAP * NEXP), BF16),
                pltpu.VMEM((4, 2 * CAP * NEXP, CB), BF16),
                pltpu.VMEM((8, TOK), jnp.int32),
                pltpu.VMEM((8, TOK), F32),
                pltpu.VMEM((4, 2, 16, 128), F32),
                dma((NSLOT,)),
                dma((4,)),
                dma((2, 4, 2, 2)),
                dma((2, 4, 2, 2)),
                dma((7,)),
                dma((4, 2)),
                dma((NCB, 2)),
                dma((NCB, 2)),
                dma((NCB, 2)),
                dma((NCB, 2)),
                dma((NCB, 2)),
                dma((NCB, 2)),
            ],
            compiler_params=pltpu.CompilerParams(collective_id=0, has_side_effects=True,
                                                 vmem_limit_bytes=66000000),
            name='moe_decode',
        )(x_loc, ids_loc.T, gates_loc.T, w_g, w_u, w_d)

    tok_spec = P(TOKEN_AXES, None)
    w_spec = P(EXPERT_AXES, None, None)
    return jax.shard_map(local_layer, mesh=mesh, in_specs=(tok_spec, tok_spec, tok_spec, w_spec, w_spec, w_spec), out_specs=tok_spec, check_vma=False)
```

```python
import jax
import jax.numpy as jnp
from jax import lax
from jax.experimental import pallas as pl
from jax.experimental.pallas import tpu as pltpu
from jax.sharding import PartitionSpec as P

TOKEN_AXES = ('ez', 'ey', 'ex')
EXPERT_AXES = ('ex', 'ey', 'ez')
MESH = pl.DeviceIdType.MESH
F32 = jnp.float32
BF16 = jnp.bfloat16

TOK = 64
HALF = TOK // 2
HID = 2048
FFN = 1024
NEXP = 8
CAP = 16
NSLOT = 10
CB = 256
NCB = HID // CB
N13 = 2 * NEXP

PEERS = [(c, s) for c in range(4) for s in range(2) if (c, s) != (0, 0)]
STAY = ((0, 2), (0, 1))
LEAVE = ((1, 3), (2, 3))
HOP1 = (1, 2)
HOP2 = (2, 1)


def kernel(x_hbm, ids_hbm, gates_hbm, wg_hbm, wu_hbm, wd_hbm, y_ref,
           ring, xs, xe, hbuf, act, drecv, r2, r3, pmat, gtmp, gmat, obuf, ids_v, gates_v, meta,
           w_sem, loc_sem, xsend, xrecv, msend, mrecv, d_send, d_recv, s2_send, s2_recv, s3_send, s3_recv):
    ez, ey, ex = lax.axis_index('ez'), lax.axis_index('ey'), lax.axis_index('ex')

    def dev(c, s):
        return (1 - ez if c & 2 else ez, 1 - ey if c & 1 else ey, 1 - ex if s else ex)

    def remote(src, dst, ssem, rsem, c, s):
        return pltpu.make_async_remote_copy(src_ref=src, dst_ref=dst, send_sem=ssem, recv_sem=rsem,
                                            device_id=dev(c, s), device_id_type=MESH)

    cp_x = [pltpu.make_async_copy(x_hbm.at[:, pl.ds(k * FFN, FFN)], xs.at[k, 0, pl.ds(0, TOK)], loc_sem.at[k])
            for k in range(2)]
    cp_i = pltpu.make_async_copy(ids_hbm, ids_v, loc_sem.at[2])
    cp_g = pltpu.make_async_copy(gates_hbm, gates_v, loc_sem.at[3])
    for cp in (cp_x[0], cp_i, cp_g, cp_x[1]):
        cp.start()

    barrier = pltpu.get_barrier_semaphore()
    for c, s in PEERS:
        pl.semaphore_signal(barrier, inc=1, device_id=dev(c, s), device_id_type=MESH)

    def start_w13(k, e, slot):
        for i, w_hbm in enumerate((wg_hbm, wu_hbm)):
            for q in range(4):
                pltpu.make_async_copy(w_hbm.at[e, k, :, pl.ds(q * CB, CB)], ring.at[slot, 4 * i + q],
                                      w_sem.at[slot]).start()

    def start_w2(cb, slot):
        cols = pl.ds(pl.multiple_of(cb * CB, CB), CB)
        for e in range(NEXP):
            pltpu.make_async_copy(wd_hbm.at[e, :, cols], ring.at[slot, e],
                                  w_sem.at[slot]).start()

    def wait_w(slot):
        pltpu.make_async_copy(ring.at[slot], ring.at[slot], w_sem.at[slot]).wait()

    def wcols(slot, i):
        return ring[slot, i]

    def start_units(first, last):
        for u in range(first, last):
            start_w13(u // NEXP, u % NEXP, u)

    start_units(0, 4)

    cp_i.wait()
    cp_g.wait()
    ids_f = ids_v[...].astype(F32)
    gates_f = gates_v[...]
    meta[0, 0, 0:8, :] = jnp.concatenate([ids_f, ids_f], axis=1)
    meta[0, 0, 8:16, :] = jnp.concatenate([gates_f, gates_f], axis=1)
    cp_x[0].wait()
    cp_x[1].wait()
    pl.semaphore_wait(barrier, len(PEERS))

    def rows(k, c, s, h):
        return xs.at[k, c, pl.ds(s * TOK + h * HALF, HALF)]

    def row_copy(k, src, dst, c, s):
        return remote(rows(k, *src), rows(k, *dst), xsend.at[k, dst[0], dst[1], dst[2]],
                      xrecv.at[k, dst[0], dst[1], dst[2]], c, s)

    ROUTES = {}
    for c in (1, 2):
        for h in range(2):
            ROUTES[(c, 0, h)] = ((0, 0, h), c, 0)
    ROUTES[(3, 0, 1)] = ((1, 0, 1), 2, 0)
    ROUTES[(3, 0, 0)] = ((2, 0, 0), 1, 0)
    for c in range(4):
        for h in range(2):
            ROUTES[(c, 1, h)] = ((c, 0, h), 0, 1)

    def send_rows(k, *dst):
        src, c, s = ROUTES[dst]
        row_copy(k, src, dst, c, s).start()

    def wait_rows(k, *dst):
        src, c, s = ROUTES[dst]
        row_copy(k, src, dst, c, s).wait_recv()

    def send_first(k):
        send_rows(k, 1, 0, 1)
        send_rows(k, 2, 0, 0)

    def send_second(k):
        send_rows(k, 1, 0, 0)
        send_rows(k, 2, 0, 1)
        send_rows(k, 0, 1, 0)
        send_rows(k, 0, 1, 1)

    def forward_first(k):
        wait_rows(k, 1, 0, 1)
        send_rows(k, 3, 0, 1)
        send_rows(k, 1, 1, 1)
        wait_rows(k, 2, 0, 0)
        send_rows(k, 3, 0, 0)
        send_rows(k, 2, 1, 0)

    def forward_second(k):
        wait_rows(k, 1, 0, 0)
        send_rows(k, 1, 1, 0)
        wait_rows(k, 2, 0, 1)
        send_rows(k, 2, 1, 1)

    def forward_third(k):
        for h in range(2):
            wait_rows(k, 3, 0, h)
            send_rows(k, 3, 1, h)

    meta_sends = []
    for i, (c, s) in enumerate(PEERS):
        cp = remote(meta.at[0, 0], meta.at[c, s], msend.at[i], mrecv.at[c, s], c, s)
        cp.start()
        meta_sends.append(cp)
    send_first(0)
    send_second(0)
    forward_first(0)
    start_units(4, 6)
    send_first(1)
    send_second(1)

    for c, s in PEERS:
        remote(meta.at[c, s], meta.at[c, s], msend.at[0], mrecv.at[c, s], 0, 1).wait_recv()
    base = ((ex * 2 + ey) * 2 + ez) * NEXP
    sub8 = lax.broadcasted_iota(jnp.int32, (NEXP, 128), 0)
    lane8 = lax.broadcasted_iota(jnp.int32, (NEXP, 128), 1)
    mine = (sub8 + base).astype(F32)
    masks, gates = [], []
    for c in range(4):
        m = jnp.where(lane8[0:1] < TOK, meta[c, 0], meta[c, 1])
        mask = jnp.zeros((NEXP, 128), F32)
        gate = jnp.zeros((NEXP, 128), F32)
        for j in range(8):
            hit = m[j:j + 1, :] == mine
            mask += jnp.where(hit, 1.0, 0.0)
            gate += jnp.where(hit, m[8 + j:9 + j, :], 0.0)
        masks.append(mask)
        gates.append(gate)
    r_i = lax.broadcasted_iota(jnp.int32, (128, 128), 0)
    c_i = lax.broadcasted_iota(jnp.int32, (128, 128), 1)
    before = jnp.where((r_i < c_i) & ((r_i < TOK) == (c_i < TOK)), 1.0, 0.0).astype(BF16)
    rank = jnp.dot(jnp.concatenate(masks, axis=0).astype(BF16), before, preferred_element_type=F32)
    sub32 = lax.broadcasted_iota(jnp.int32, (2 * CAP, 128), 0).astype(F32)
    core_off = jnp.where(lane8 < TOK, 0.0, float(CAP))
    for c in range(4):
        code = jnp.where(masks[c] > 0.5, rank[c * NEXP:(c + 1) * NEXP] + core_off, -1.0)
        for e in range(NEXP):
            hit = sub32 == code[e:e + 1, :]
            pmat[c, 2 * CAP * e:2 * CAP * (e + 1), :] = jnp.where(hit, 1.0, 0.0).astype(BF16)
            gtmp[c, 2 * CAP * e:2 * CAP * (e + 1), :] = jnp.where(hit, gates[c][e:e + 1, :], 0.0)
    for c in range(4):
        gt = gtmp[c].T
        hi = gt.astype(BF16)
        rest = gt - hi.astype(F32)
        mid = rest.astype(BF16)
        gmat[c, 0:128, :] = hi
        gmat[c, 128:256, :] = mid
        gmat[c, 256:384, :] = (rest - mid.astype(F32)).astype(BF16)

    def gather(k, c):
        for h in range(2):
            if (c, 1, h) in ROUTES:
                wait_rows(k, c, 1, h)
        for nb in range(FFN // 512):
            cols = slice(nb * 512, (nb + 1) * 512)
            blk = jnp.dot(pmat[c], xs[k, c, :, cols], preferred_element_type=F32).astype(BF16)
            for e in range(NEXP):
                xe[k, e, 2 * CAP * c:2 * CAP * (c + 1), cols] = blk[2 * CAP * e:2 * CAP * (e + 1)]

    gather(0, 0)
    forward_second(0)
    start_units(6, 8)
    gather(0, 1)
    gather(0, 2)
    start_units(8, NSLOT)
    forward_third(0)
    gather(0, 3)

    def refill(u, slot):
        nxt = u + NSLOT

        @pl.when(nxt < N13)
        def _():
            start_w13(nxt // NEXP, lax.rem(nxt, NEXP), slot)

        @pl.when((nxt >= N13) & (nxt < N13 + NCB))
        def _():
            start_w2(nxt - N13, slot)

    def up0(e, carry):
        slot = lax.rem(e, NSLOT)
        wait_w(slot)
        for q in range(8):
            hbuf[e, q] = jnp.dot(xe[0, e], wcols(slot, q), preferred_element_type=F32)
        refill(e, slot)

        @pl.when(e == 0)
        def _():
            forward_first(1)

        @pl.when(e == 2)
        def _():
            forward_second(1)
            gather(1, 0)

        @pl.when(e == 5)
        def _():
            gather(1, 1)
            gather(1, 2)
            forward_third(1)

        return carry

    lax.fori_loop(0, NEXP, up0, 0)
    gather(1, 3)

    def up1(e, carry):
        u = e + NEXP
        slot = lax.rem(u, NSLOT)
        wait_w(slot)
        for q in range(4):
            h1 = hbuf[e, q] + jnp.dot(xe[1, e], wcols(slot, q), preferred_element_type=F32)
            h3 = hbuf[e, 4 + q] + jnp.dot(xe[1, e], wcols(slot, 4 + q), preferred_element_type=F32)
            act[e, :, q * CB:(q + 1) * CB] = (jax.nn.silu(h1) * h3).astype(BF16)
        refill(u, slot)
        return carry

    lax.fori_loop(0, NEXP, up1, 0)

    def d_copy(cb, g):
        return remote(hbuf.at[cb, g], drecv.at[cb, g], d_send.at[cb, g], d_recv.at[cb, g], 0, 1)

    def s2_copy(cb, h):
        return remote(hbuf.at[cb, 3, pl.ds(h * TOK, TOK)], r2.at[cb, pl.ds(h * TOK, TOK)],
                      s2_send.at[cb, h], s2_recv.at[cb, h], HOP1[h], 0)

    def s3_copy(cb, h):
        return remote(hbuf.at[cb, 2, pl.ds(h * TOK + HALF, HALF)], r3.at[cb, pl.ds(h * HALF, HALF)],
                      s3_send.at[cb, h], s3_recv.at[cb, h], HOP2[h], 0)

    def part(cb):
        slot = lax.rem(N13 + cb, NSLOT)
        wait_w(slot)
        for e in range(NEXP):
            o = jnp.dot(act[e], wcols(slot, e), preferred_element_type=F32).astype(BF16)
            for c in range(4):
                obuf[c, 2 * CAP * e:2 * CAP * (e + 1), :] = o[2 * CAP * c:2 * CAP * (c + 1)]
        for c in (3, 1, 2, 0):
            t = jnp.dot(gmat[c], obuf[c], preferred_element_type=F32)
            t = t[0:128] + t[128:256] + t[256:384]
            for h in range(2):
                g = 0 if c in STAY[h] else 1
                place = (LEAVE if g else STAY)[h].index(c)
                at = pl.ds(h * TOK + place * HALF, HALF)
                hbuf[cb, 2 + g, at] = t[h * HALF:(h + 1) * HALF]
                hbuf[cb, g, at] = t[TOK + h * HALF:TOK + (h + 1) * HALF]
        d_copy(cb, 1).start()
        d_copy(cb, 0).start()

    def stage2(cb):
        d_copy(cb, 1).wait_recv()
        hbuf[cb, 3] = hbuf[cb, 3] + drecv[cb, 1]
        s2_copy(cb, 0).start()
        s2_copy(cb, 1).start()

    def down(cb, carry):
        part(cb)

        @pl.when(cb > 0)
        def _():
            stage2(cb - 1)

        return carry

    lax.fori_loop(0, NCB, down, 0)
    stage2(NCB - 1)

    def third(cb, carry):
        d_copy(cb, 0).wait_recv()
        for h in range(2):
            s2_copy(cb, h).wait_recv()
        hbuf[cb, 2] = (hbuf[cb, 2] + drecv[cb, 0]) + r2[cb]
        for h in range(2):
            s3_copy(cb, h).start()
        return carry

    lax.fori_loop(0, NCB, third, 0)

    def last(cb, carry):
        cols = pl.ds(pl.multiple_of(lax.rem(cb, 4) * CB, CB), CB)
        ycols = pl.ds(pl.multiple_of(cb * CB, CB), CB)
        for h in range(2):
            s3_copy(cb, h).wait_recv()
            at = pl.ds(h * HALF, HALF)
            xin = xs[cb // 4, 0, at, cols].astype(F32)
            y_ref[at, ycols] = (xin + (hbuf[cb, 2, pl.ds(h * TOK, HALF)] + r3[cb, at])).astype(BF16)
        return carry

    lax.fori_loop(0, NCB, last, 0)

    for cp in meta_sends:
        cp.wait_send()
    for k in range(2):
        for dst, (src, c, s) in ROUTES.items():
            row_copy(k, src, dst, c, s).wait_send()
    for cb in range(NCB):
        for i in range(2):
            d_copy(cb, i).wait_send()
            s2_copy(cb, i).wait_send()
            s3_copy(cb, i).wait_send()


def solution(mesh):
    def local_layer(x_loc, ids_loc, gates_loc, w_g, w_u, w_d):
        w_g = w_g.reshape(NEXP, 2, FFN, FFN)
        w_u = w_u.reshape(NEXP, 2, FFN, FFN)
        any_spec = pl.BlockSpec(memory_space=pl.ANY)
        dma = pltpu.SemaphoreType.DMA
        return pl.pallas_call(
            kernel,
            out_shape=pltpu.VMEM((TOK, HID), BF16),
            in_specs=[any_spec] * 6,
            out_specs=pl.BlockSpec(memory_space=pltpu.VMEM),
            scratch_shapes=[
                pltpu.VMEM((NSLOT, NEXP, FFN, CB), BF16),
                pltpu.VMEM((2, 4, 2 * TOK, FFN), BF16),
                pltpu.VMEM((2, NEXP, 8 * CAP, FFN), BF16),
                pltpu.VMEM((NEXP, 8, 8 * CAP, CB), F32),
                pltpu.VMEM((NEXP, 8 * CAP, FFN), BF16),
                pltpu.VMEM((NCB, 2, 2 * TOK, CB), F32),
                pltpu.VMEM((NCB, 2 * TOK, CB), F32),
                pltpu.VMEM((NCB, TOK, CB), F32),
                pltpu.VMEM((4, 2 * CAP * NEXP, 128), BF16),
                pltpu.VMEM((4, 2 * CAP * NEXP, 128), F32),
                pltpu.VMEM((4, 384, 2 * CAP * NEXP), BF16),
                pltpu.VMEM((4, 2 * CAP * NEXP, CB), BF16),
                pltpu.VMEM((8, TOK), jnp.int32),
                pltpu.VMEM((8, TOK), F32),
                pltpu.VMEM((4, 2, 16, 128), F32),
                dma((NSLOT,)),
                dma((4,)),
                dma((2, 4, 2, 2)),
                dma((2, 4, 2, 2)),
                dma((7,)),
                dma((4, 2)),
                dma((NCB, 2)),
                dma((NCB, 2)),
                dma((NCB, 2)),
                dma((NCB, 2)),
                dma((NCB, 2)),
                dma((NCB, 2)),
            ],
            compiler_params=pltpu.CompilerParams(collective_id=0, has_side_effects=True,
                                                 vmem_limit_bytes=66000000),
            name='moe_decode',
        )(x_loc, ids_loc.T, gates_loc.T, w_g, w_u, w_d)

    tok_spec = P(TOKEN_AXES, None)
    w_spec = P(EXPERT_AXES, None, None)
    return jax.shard_map(local_layer, mesh=mesh, in_specs=(tok_spec, tok_spec, tok_spec, w_spec, w_spec, w_spec), out_specs=tok_spec, check_vma=False)
```

```python
import jax
import jax.numpy as jnp
from jax import lax
from jax.experimental import pallas as pl
from jax.experimental.pallas import tpu as pltpu
from jax.sharding import PartitionSpec as P

TOKEN_AXES = ('ez', 'ey', 'ex')
EXPERT_AXES = ('ex', 'ey', 'ez')
MESH = pl.DeviceIdType.MESH
F32 = jnp.float32
BF16 = jnp.bfloat16

TOK = 64
HALF = TOK // 2
Q = TOK // 4
HID = 2048
FFN = 1024
NEXP = 8
CAP = 16
NSLOT = 10
CB = 256
NCB = HID // CB
N13 = 2 * NEXP

PEERS = [(c, s) for c in range(4) for s in range(2) if (c, s) != (0, 0)]
STAY = ((0, 2), (0, 1))
LEAVE = ((1, 3), (2, 3))
HOP1 = (1, 2)
HOP2 = (2, 1)


def kernel(x_hbm, ids_hbm, gates_hbm, wg_hbm, wu_hbm, wd_hbm, y_ref,
           ring, xs, xe, hbuf, act, drecv, r2, r3, pmat, gtmp, gmat, obuf, ids_v, gates_v, meta,
           w_sem, loc_sem, xsend, xa, xb, xd, drows, msend, mrecv, d_send, d_recv, d_stay, s2_send, s2_recv, s3_send, s3_recv):
    ez, ey, ex = lax.axis_index('ez'), lax.axis_index('ey'), lax.axis_index('ex')

    def dev(c, s):
        return (1 - ez if c & 2 else ez, 1 - ey if c & 1 else ey, 1 - ex if s else ex)

    def remote(src, dst, ssem, rsem, c, s):
        return pltpu.make_async_remote_copy(src_ref=src, dst_ref=dst, send_sem=ssem, recv_sem=rsem,
                                            device_id=dev(c, s), device_id_type=MESH)

    cp_x = [pltpu.make_async_copy(x_hbm.at[:, pl.ds(k * FFN, FFN)], xs.at[k, 0, pl.ds(0, TOK)], loc_sem.at[k])
            for k in range(2)]
    cp_i = pltpu.make_async_copy(ids_hbm, ids_v, loc_sem.at[2])
    cp_g = pltpu.make_async_copy(gates_hbm, gates_v, loc_sem.at[3])
    for cp in (cp_x[0], cp_i, cp_g, cp_x[1]):
        cp.start()

    barrier = pltpu.get_barrier_semaphore()
    for c, s in PEERS:
        pl.semaphore_signal(barrier, inc=1, device_id=dev(c, s), device_id_type=MESH)

    def start_w13(k, e, slot):
        for i, w_hbm in enumerate((wg_hbm, wu_hbm)):
            for q in range(4):
                pltpu.make_async_copy(w_hbm.at[e, k, :, pl.ds(q * CB, CB)], ring.at[slot, 4 * i + q],
                                      w_sem.at[slot]).start()

    def start_w2(cb, slot):
        cols = pl.ds(pl.multiple_of(cb * CB, CB), CB)
        for e in range(NEXP):
            pltpu.make_async_copy(wd_hbm.at[e, :, cols], ring.at[slot, e],
                                  w_sem.at[slot]).start()

    def wait_w(slot):
        pltpu.make_async_copy(ring.at[slot], ring.at[slot], w_sem.at[slot]).wait()

    def wcols(slot, i):
        return ring[slot, i]

    def start_units(first, last):
        for u in range(first, last):
            start_w13(u // NEXP, u % NEXP, u)

    start_units(0, 6)

    cp_i.wait()
    cp_g.wait()
    ids_f = ids_v[...].astype(F32)
    gates_f = gates_v[...]
    meta[0] = jnp.concatenate([ids_f, gates_f], axis=1)
    cp_x[0].wait()
    pl.semaphore_wait(barrier, len(PEERS))

    def send_rows(k, src, dst, first, count, rsem, c, s):
        at = lambda cc, ss: xs.at[k, cc, pl.ds(ss * TOK + first, count)]
        remote(at(*src), at(*dst), xsend.at[0], rsem, c, s).start()

    def wait_all(ref, sem):
        pltpu.make_async_copy(ref, ref, sem).wait()

    def wait_rows(k, c, first, count, sem):
        wait_all(xs.at[k, c, pl.ds(first, count)], sem)

    def across(k, c, first, count):
        send_rows(k, (c, 0), (c, 1), first, count, drows.at[k, c // 3], 0, 1)

    def fwd_first(c, i):
        return (HALF if c == 1 else 0) + i * Q

    def send_first(k):
        for i in range(2):
            for c in (1, 2):
                send_rows(k, (0, 0), (c, 0), fwd_first(c, i), Q, xa.at[k, c - 1, i], c, 0)

    def send_second(k):
        for c in (1, 2):
            send_rows(k, (0, 0), (c, 0), HALF - fwd_first(c, 0), HALF, xb.at[k, c - 1], c, 0)
        across(k, 0, 0, TOK)

    def forward_first(k):
        for i in range(2):
            for c in (1, 2):
                wait_rows(k, c, fwd_first(c, i), Q, xa.at[k, c - 1, i])
                send_rows(k, (c, 0), (3, 0), fwd_first(c, i), Q, xd.at[k, c - 1, i], 3 - c, 0)
        for c in (1, 2):
            across(k, c, fwd_first(c, 0), HALF)

    def forward_second(k):
        for c in (1, 2):
            first = HALF - fwd_first(c, 0)
            wait_rows(k, c, first, HALF, xb.at[k, c - 1])
            across(k, c, first, HALF)

    def forward_third(k):
        for i in range(2):
            for c in (1, 2):
                wait_rows(k, 3, fwd_first(c, i), Q, xd.at[k, c - 1, i])
                across(k, 3, fwd_first(c, i), Q)

    send_first(0)
    for c, s in PEERS:
        remote(meta.at[0], meta.at[2 * c + s], msend.at[0], mrecv.at[0], c, s).start()
    send_second(0)
    forward_first(0)
    start_units(6, NSLOT)
    cp_x[1].wait()
    send_first(1)
    send_second(1)

    wait_all(meta.at[pl.ds(1, 7)], mrecv.at[0])
    base = ((ex * 2 + ey) * 2 + ez) * NEXP
    sub8 = lax.broadcasted_iota(jnp.int32, (NEXP, 128), 0)
    lane8 = lax.broadcasted_iota(jnp.int32, (NEXP, 128), 1)
    mine = (sub8 + base).astype(F32)
    masks, gates = [], []
    for c in range(4):
        m0, m1 = meta[2 * c], meta[2 * c + 1]
        ids_c = jnp.where(lane8 < TOK, m0, pltpu.roll(m1, TOK, 1))
        gates_c = jnp.where(lane8 < TOK, pltpu.roll(m0, TOK, 1), m1)
        mask = jnp.zeros((NEXP, 128), F32)
        gate = jnp.zeros((NEXP, 128), F32)
        for j in range(8):
            hit = ids_c[j:j + 1, :] == mine
            mask += jnp.where(hit, 1.0, 0.0)
            gate += jnp.where(hit, gates_c[j:j + 1, :], 0.0)
        masks.append(mask)
        gates.append(gate)
    r_i = lax.broadcasted_iota(jnp.int32, (128, 128), 0)
    c_i = lax.broadcasted_iota(jnp.int32, (128, 128), 1)
    before = jnp.where((r_i < c_i) & ((r_i < TOK) == (c_i < TOK)), 1.0, 0.0).astype(BF16)
    rank = jnp.dot(jnp.concatenate(masks, axis=0).astype(BF16), before, preferred_element_type=F32)
    sub32 = lax.broadcasted_iota(jnp.int32, (2 * CAP, 128), 0).astype(F32)
    core_off = jnp.where(lane8 < TOK, 0.0, float(CAP))
    for c in range(4):
        code = jnp.where(masks[c] > 0.5, rank[c * NEXP:(c + 1) * NEXP] + core_off, -1.0)
        for e in range(NEXP):
            hit = sub32 == code[e:e + 1, :]
            pmat[c, 2 * CAP * e:2 * CAP * (e + 1), :] = jnp.where(hit, 1.0, 0.0).astype(BF16)
            gtmp[c, 2 * CAP * e:2 * CAP * (e + 1), :] = jnp.where(hit, gates[c][e:e + 1, :], 0.0)
    for c in range(4):
        gt = gtmp[c].T
        hi = gt.astype(BF16)
        rest = gt - hi.astype(F32)
        mid = rest.astype(BF16)
        gmat[c, 0:128, :] = hi
        gmat[c, 128:256, :] = mid
        gmat[c, 256:384, :] = (rest - mid.astype(F32)).astype(BF16)

    def gather(k, c):
        for nb in range(FFN // 512):
            cols = slice(nb * 512, (nb + 1) * 512)
            blk = jnp.dot(pmat[c], xs[k, c, :, cols], preferred_element_type=F32).astype(BF16)
            for e in range(NEXP):
                xe[k, e, 2 * CAP * c:2 * CAP * (c + 1), cols] = blk[2 * CAP * e:2 * CAP * (e + 1)]

    def gather_near(k):
        wait_all(xs.at[k, pl.ds(0, 3), pl.ds(TOK, TOK)], drows.at[k, 0])
        for c in range(3):
            gather(k, c)

    def gather_far(k):
        wait_all(xs.at[k, 3, pl.ds(TOK, TOK)], drows.at[k, 1])
        gather(k, 3)

    forward_second(0)
    gather_near(0)
    forward_third(0)
    gather_far(0)

    def refill(u, slot):
        nxt = u + NSLOT

        @pl.when(nxt < N13)
        def _():
            start_w13(nxt // NEXP, lax.rem(nxt, NEXP), slot)

        @pl.when((nxt >= N13) & (nxt < N13 + NCB))
        def _():
            start_w2(nxt - N13, slot)

    def up0(i, carry):
        for j in range(2):
            wait_w(lax.rem(2 * i + j, NSLOT))
        for j in range(2):
            e = 2 * i + j
            for q in range(8):
                hbuf[e, q] = jnp.dot(xe[0, e], wcols(lax.rem(e, NSLOT), q), preferred_element_type=F32)
        for j in range(2):
            refill(2 * i + j, lax.rem(2 * i + j, NSLOT))

        @pl.when(i == 0)
        def _():
            forward_first(1)

        @pl.when(i == 1)
        def _():
            forward_second(1)

        @pl.when(i == 2)
        def _():
            gather_near(1)
            forward_third(1)

        return carry

    lax.fori_loop(0, NEXP // 2, up0, 0)
    gather_far(1)

    def up1(e, carry):
        u = e + NEXP
        slot = lax.rem(u, NSLOT)
        wait_w(slot)
        for q in range(4):
            h1 = hbuf[e, q] + jnp.dot(xe[1, e], wcols(slot, q), preferred_element_type=F32)
            h3 = hbuf[e, 4 + q] + jnp.dot(xe[1, e], wcols(slot, 4 + q), preferred_element_type=F32)
            act[e, :, q * CB:(q + 1) * CB] = (jax.nn.silu(h1) * h3).astype(BF16)
        refill(u, slot)
        return carry

    lax.fori_loop(0, NEXP, up1, 0)

    wait_all(hbuf.at[pl.ds(0, 2), pl.ds(0, 7)], xsend.at[0])
    wait_all(meta.at[pl.ds(1, 7)], msend.at[0])

    def d_copy(cb, g):
        return remote(hbuf.at[cb, g], drecv.at[cb, g], d_send.at[0], d_recv.at[cb] if g else d_stay.at[0], 0, 1)

    def s2_copy(cb, h):
        return remote(hbuf.at[cb, 3, pl.ds(h * TOK, TOK)], r2.at[cb, pl.ds(h * TOK, TOK)],
                      s2_send.at[0], s2_recv.at[cb // 2], HOP1[h], 0)

    def s3_copy(i, h):
        return remote(hbuf.at[pl.ds(2 * i, 2), 2, pl.ds(h * TOK + HALF, HALF)],
                      r3.at[pl.ds(2 * i, 2), pl.ds(h * HALF, HALF)],
                      s3_send.at[0], s3_recv.at[(i + 1) // (NCB // 2)], HOP2[h], 0)

    def part(cb):
        slot = lax.rem(N13 + cb, NSLOT)
        wait_w(slot)
        for e in range(NEXP):
            o = jnp.dot(act[e], wcols(slot, e), preferred_element_type=F32).astype(BF16)
            for c in range(4):
                obuf[c, 2 * CAP * e:2 * CAP * (e + 1), :] = o[2 * CAP * c:2 * CAP * (c + 1)]
        for c in (3, 1, 2, 0):
            t = jnp.dot(gmat[c], obuf[c], preferred_element_type=F32)
            t = t[0:128] + t[128:256] + t[256:384]
            for h in range(2):
                g = 0 if c in STAY[h] else 1
                place = (LEAVE if g else STAY)[h].index(c)
                at = pl.ds(h * TOK + place * HALF, HALF)
                hbuf[cb, 2 + g, at] = t[h * HALF:(h + 1) * HALF]
                hbuf[cb, g, at] = t[TOK + h * HALF:TOK + (h + 1) * HALF]
        d_copy(cb, 1).start()
        d_copy(cb, 0).start()

    def stage2(cb):
        d_copy(cb, 1).wait_recv()
        hbuf[cb, 3] = hbuf[cb, 3] + drecv[cb, 1]
        s2_copy(cb, 0).start()
        s2_copy(cb, 1).start()

    def down(cb, carry):
        part(cb)

        @pl.when(cb > 0)
        def _():
            stage2(cb - 1)

        return carry

    lax.fori_loop(0, NCB, down, 0)
    stage2(NCB - 1)

    wait_all(drecv.at[:, 0], d_stay.at[0])

    def third(i, carry):
        pair = pl.ds(2 * i, 2)
        wait_all(r2.at[pair], s2_recv.at[i])
        hbuf[pair, 2] = (hbuf[pair, 2] + drecv[pair, 0]) + r2[pair]
        for h in range(2):
            s3_copy(i, h).start()
        return carry

    lax.fori_loop(0, NCB // 2, third, 0)
    wait_all(drecv, d_send.at[0])
    wait_all(r2, s2_send.at[0])

    def last(cb, carry):
        cols = pl.ds(pl.multiple_of(lax.rem(cb, 4) * CB, CB), CB)
        ycols = pl.ds(pl.multiple_of(cb * CB, CB), CB)
        for h in range(2):
            at = pl.ds(h * HALF, HALF)
            xin = xs[cb // 4, 0, at, cols].astype(F32)
            y_ref[at, ycols] = (xin + (hbuf[cb, 2, pl.ds(h * TOK, HALF)] + r3[cb, at])).astype(BF16)
        return carry

    wait_all(r3.at[pl.ds(0, NCB - 2)], s3_recv.at[0])
    lax.fori_loop(0, NCB - 2, last, 0)
    wait_all(r3.at[pl.ds(NCB - 2, 2)], s3_recv.at[1])
    lax.fori_loop(NCB - 2, NCB, last, 0)
    wait_all(r3, s3_send.at[0])


def solution(mesh):
    def local_layer(x_loc, ids_loc, gates_loc, w_g, w_u, w_d):
        w_g = w_g.reshape(NEXP, 2, FFN, FFN)
        w_u = w_u.reshape(NEXP, 2, FFN, FFN)
        any_spec = pl.BlockSpec(memory_space=pl.ANY)
        dma = pltpu.SemaphoreType.DMA
        return pl.pallas_call(
            kernel,
            out_shape=pltpu.VMEM((TOK, HID), BF16),
            in_specs=[any_spec] * 6,
            out_specs=pl.BlockSpec(memory_space=pltpu.VMEM),
            scratch_shapes=[
                pltpu.VMEM((NSLOT, NEXP, FFN, CB), BF16),
                pltpu.VMEM((2, 4, 2 * TOK, FFN), BF16),
                pltpu.VMEM((2, NEXP, 8 * CAP, FFN), BF16),
                pltpu.VMEM((NEXP, 8, 8 * CAP, CB), F32),
                pltpu.VMEM((NEXP, 8 * CAP, FFN), BF16),
                pltpu.VMEM((NCB, 2, 2 * TOK, CB), F32),
                pltpu.VMEM((NCB, 2 * TOK, CB), F32),
                pltpu.VMEM((NCB, TOK, CB), F32),
                pltpu.VMEM((4, 2 * CAP * NEXP, 128), BF16),
                pltpu.VMEM((4, 2 * CAP * NEXP, 128), F32),
                pltpu.VMEM((4, 384, 2 * CAP * NEXP), BF16),
                pltpu.VMEM((4, 2 * CAP * NEXP, CB), BF16),
                pltpu.VMEM((8, TOK), jnp.int32),
                pltpu.VMEM((8, TOK), F32),
                pltpu.VMEM((8, 8, 128), F32),
                dma((NSLOT,)),
                dma((4,)),
                dma((1,)),
                dma((2, 2, 2)),
                dma((2, 2)),
                dma((2, 2, 2)),
                dma((2, 2)),
                dma((1,)),
                dma((1,)),
                dma((1,)),
                dma((NCB,)),
                dma((1,)),
                dma((1,)),
                dma((NCB // 2,)),
                dma((1,)),
                dma((2,)),
            ],
            compiler_params=pltpu.CompilerParams(collective_id=0, has_side_effects=True,
                                                 vmem_limit_bytes=66000000),
            name='moe_decode',
        )(x_loc, ids_loc.T, gates_loc.T, w_g, w_u, w_d)

    tok_spec = P(TOKEN_AXES, None)
    w_spec = P(EXPERT_AXES, None, None)
    return jax.shard_map(local_layer, mesh=mesh, in_specs=(tok_spec, tok_spec, tok_spec, w_spec, w_spec, w_spec), out_specs=tok_spec, check_vma=False)
```

```python
import jax
import jax.numpy as jnp
from jax import lax
from jax.experimental import pallas as pl
from jax.experimental.pallas import tpu as pltpu
from jax.sharding import PartitionSpec as P

TOKEN_AXES = ('ez', 'ey', 'ex')
EXPERT_AXES = ('ex', 'ey', 'ez')
MESH = pl.DeviceIdType.MESH
F32 = jnp.float32
BF16 = jnp.bfloat16

TOK = 64
HALF = TOK // 2
Q = TOK // 4
HID = 2048
FFN = 1024
NEXP = 8
CAP = 16
NSLOT = 10
CB = 256
NCB = HID // CB
N13 = 2 * NEXP

PEERS = [(c, s) for c in range(4) for s in range(2) if (c, s) != (0, 0)]
STAY = ((0, 2), (0, 1))
LEAVE = ((1, 3), (2, 3))
HOP1 = (1, 2)
HOP2 = (2, 1)


def kernel(x_hbm, ids_hbm, gates_hbm, wg_hbm, wu_hbm, wd_hbm, y_ref,
           ring, xs, xe, hbuf, act, drecv, r2, r3, pmat, gtmp, gmat, obuf, ids_v, gates_v, meta,
           w_sem, loc_sem, xsend, xa, xb, xd, drows, msend, mrecv, d_send, d_recv, d_stay, s2_send, s2_recv, s3_send, s3_recv):
    ez, ey, ex = lax.axis_index('ez'), lax.axis_index('ey'), lax.axis_index('ex')

    def dev(c, s):
        return (1 - ez if c & 2 else ez, 1 - ey if c & 1 else ey, 1 - ex if s else ex)

    def remote(src, dst, ssem, rsem, c, s):
        return pltpu.make_async_remote_copy(src_ref=src, dst_ref=dst, send_sem=ssem, recv_sem=rsem,
                                            device_id=dev(c, s), device_id_type=MESH)

    cp_x = [pltpu.make_async_copy(x_hbm.at[:, pl.ds(k * FFN, FFN)], xs.at[k, 0, pl.ds(0, TOK)], loc_sem.at[k])
            for k in range(2)]
    cp_i = pltpu.make_async_copy(ids_hbm, ids_v, loc_sem.at[2])
    cp_g = pltpu.make_async_copy(gates_hbm, gates_v, loc_sem.at[3])
    for cp in (cp_x[0], cp_i, cp_g, cp_x[1]):
        cp.start()

    barrier = pltpu.get_barrier_semaphore()
    for c, s in PEERS:
        pl.semaphore_signal(barrier, inc=1, device_id=dev(c, s), device_id_type=MESH)

    def start_w13(k, e, slot):
        for i, w_hbm in enumerate((wg_hbm, wu_hbm)):
            for q in range(4):
                pltpu.make_async_copy(w_hbm.at[e, k, :, pl.ds(q * CB, CB)], ring.at[slot, 4 * i + q],
                                      w_sem.at[slot]).start()

    def start_w2(cb, slot):
        cols = pl.ds(pl.multiple_of(cb * CB, CB), CB)
        for e in range(NEXP):
            pltpu.make_async_copy(wd_hbm.at[e, :, cols], ring.at[slot, e],
                                  w_sem.at[slot]).start()

    def wait_w(slot):
        pltpu.make_async_copy(ring.at[slot], ring.at[slot], w_sem.at[slot]).wait()

    def wcols(slot, i):
        return ring[slot, i]

    def start_units(first, last):
        for u in range(first, last):
            start_w13(u // NEXP, u % NEXP, u)

    start_units(0, 6)

    cp_i.wait()
    cp_g.wait()
    ids_f = ids_v[...].astype(F32)
    gates_f = gates_v[...]
    meta[0] = jnp.concatenate([ids_f, gates_f], axis=1)
    cp_x[0].wait()
    pl.semaphore_wait(barrier, len(PEERS))

    def send_rows(k, src, dst, first, count, rsem, c, s):
        at = lambda cc, ss: xs.at[k, cc, pl.ds(ss * TOK + first, count)]
        remote(at(*src), at(*dst), xsend.at[0], rsem, c, s).start()

    def wait_all(ref, sem):
        pltpu.make_async_copy(ref, ref, sem).wait()

    def wait_rows(k, c, first, count, sem):
        wait_all(xs.at[k, c, pl.ds(first, count)], sem)

    def across(k, c, first, count):
        send_rows(k, (c, 0), (c, 1), first, count, drows.at[k, c // 3], 0, 1)

    def fwd_first(c, i):
        return (HALF if c == 1 else 0) + i * Q

    def send_first(k):
        for i in range(2):
            for c in (1, 2):
                send_rows(k, (0, 0), (c, 0), fwd_first(c, i), Q, xa.at[k, c - 1, i], c, 0)

    def send_second(k):
        for c in (1, 2):
            send_rows(k, (0, 0), (c, 0), HALF - fwd_first(c, 0), HALF, xb.at[k, c - 1], c, 0)
        across(k, 0, 0, TOK)

    def forward_first(k):
        for i in range(2):
            for c in (1, 2):
                wait_rows(k, c, fwd_first(c, i), Q, xa.at[k, c - 1, i])
                send_rows(k, (c, 0), (3, 0), fwd_first(c, i), Q, xd.at[k, c - 1, i], 3 - c, 0)
        for c in (1, 2):
            across(k, c, fwd_first(c, 0), HALF)

    def forward_second(k):
        for c in (1, 2):
            first = HALF - fwd_first(c, 0)
            wait_rows(k, c, first, HALF, xb.at[k, c - 1])
            across(k, c, first, HALF)

    def forward_third(k):
        for i in range(2):
            for c in (1, 2):
                wait_rows(k, 3, fwd_first(c, i), Q, xd.at[k, c - 1, i])
                across(k, 3, fwd_first(c, i), Q)

    send_first(0)
    for c, s in PEERS:
        remote(meta.at[0], meta.at[2 * c + s], msend.at[0], mrecv.at[0], c, s).start()
    send_second(0)
    forward_first(0)
    start_units(6, NSLOT)
    cp_x[1].wait()
    send_first(1)
    send_second(1)

    wait_all(meta.at[pl.ds(1, 7)], mrecv.at[0])
    base = ((ex * 2 + ey) * 2 + ez) * NEXP
    sub8 = lax.broadcasted_iota(jnp.int32, (NEXP, 128), 0)
    lane8 = lax.broadcasted_iota(jnp.int32, (NEXP, 128), 1)
    mine = (sub8 + base).astype(F32)
    masks, gates = [], []
    for c in range(4):
        m0, m1 = meta[2 * c], meta[2 * c + 1]
        ids_c = jnp.where(lane8 < TOK, m0, pltpu.roll(m1, TOK, 1))
        gates_c = jnp.where(lane8 < TOK, pltpu.roll(m0, TOK, 1), m1)
        mask = jnp.zeros((NEXP, 128), F32)
        gate = jnp.zeros((NEXP, 128), F32)
        for j in range(8):
            hit = ids_c[j:j + 1, :] == mine
            mask += jnp.where(hit, 1.0, 0.0)
            gate += jnp.where(hit, gates_c[j:j + 1, :], 0.0)
        masks.append(mask)
        gates.append(gate)
    r_i = lax.broadcasted_iota(jnp.int32, (128, 128), 0)
    c_i = lax.broadcasted_iota(jnp.int32, (128, 128), 1)
    before = jnp.where((r_i < c_i) & ((r_i < TOK) == (c_i < TOK)), 1.0, 0.0).astype(BF16)
    rank = jnp.dot(jnp.concatenate(masks, axis=0).astype(BF16), before, preferred_element_type=F32)
    sub32 = lax.broadcasted_iota(jnp.int32, (2 * CAP, 128), 0).astype(F32)
    core_off = jnp.where(lane8 < TOK, 0.0, float(CAP))
    for c in range(4):
        code = jnp.where(masks[c] > 0.5, rank[c * NEXP:(c + 1) * NEXP] + core_off, -1.0)
        for e in range(NEXP):
            hit = sub32 == code[e:e + 1, :]
            pmat[c, 2 * CAP * e:2 * CAP * (e + 1), :] = jnp.where(hit, 1.0, 0.0).astype(BF16)
            gtmp[c, 2 * CAP * e:2 * CAP * (e + 1), :] = jnp.where(hit, gates[c][e:e + 1, :], 0.0)
    for c in range(4):
        gt = gtmp[c].T
        hi = gt.astype(BF16)
        rest = gt - hi.astype(F32)
        mid = rest.astype(BF16)
        gmat[c, 0:128, :] = hi
        gmat[c, 128:256, :] = mid
        gmat[c, 256:384, :] = (rest - mid.astype(F32)).astype(BF16)

    def gather(k, c):
        for nb in range(FFN // 512):
            cols = slice(nb * 512, (nb + 1) * 512)
            blk = jnp.dot(pmat[c], xs[k, c, :, cols], preferred_element_type=F32).astype(BF16)
            for e in range(NEXP):
                xe[k, e, 2 * CAP * c:2 * CAP * (c + 1), cols] = blk[2 * CAP * e:2 * CAP * (e + 1)]

    def gather_near(k):
        wait_all(xs.at[k, pl.ds(0, 3), pl.ds(TOK, TOK)], drows.at[k, 0])
        for c in range(3):
            gather(k, c)

    def gather_far(k):
        wait_all(xs.at[k, 3, pl.ds(TOK, TOK)], drows.at[k, 1])
        gather(k, 3)

    forward_second(0)
    gather_near(0)
    forward_third(0)
    gather_far(0)

    def refill(u, slot):
        nxt = u + NSLOT

        @pl.when(nxt < N13)
        def _():
            start_w13(nxt // NEXP, lax.rem(nxt, NEXP), slot)

        @pl.when((nxt >= N13) & (nxt < N13 + NCB))
        def _():
            start_w2(nxt - N13, slot)

    def up0(i, carry):
        for j in range(2):
            wait_w(lax.rem(2 * i + j, NSLOT))
        for j in range(2):
            e = 2 * i + j
            for q in range(8):
                hbuf[e, q] = jnp.dot(xe[0, e], wcols(lax.rem(e, NSLOT), q), preferred_element_type=F32)
        for j in range(2):
            refill(2 * i + j, lax.rem(2 * i + j, NSLOT))

        @pl.when(i == 0)
        def _():
            forward_first(1)

        @pl.when(i == 1)
        def _():
            forward_second(1)

        @pl.when(i == 2)
        def _():
            gather_near(1)
            forward_third(1)

        return carry

    lax.fori_loop(0, NEXP // 2, up0, 0)
    gather_far(1)

    def up1(first, count):
        slots = [lax.rem(first + j + NEXP, NSLOT) for j in range(count)]
        for slot in slots:
            wait_w(slot)
        for j, slot in enumerate(slots):
            e = first + j
            for q in range(4):
                h1 = hbuf[e, q] + jnp.dot(xe[1, e], wcols(slot, q), preferred_element_type=F32)
                h3 = hbuf[e, 4 + q] + jnp.dot(xe[1, e], wcols(slot, 4 + q), preferred_element_type=F32)
                act[e, :, q * CB:(q + 1) * CB] = (jax.nn.silu(h1) * h3).astype(BF16)
        for j, slot in enumerate(slots):
            refill(first + j + NEXP, slot)

    def up1_pair(i, carry):
        up1(2 * i, 2)
        return carry

    def up1_one(e, carry):
        up1(e, 1)
        return carry

    lax.fori_loop(0, NEXP // 2 - 1, up1_pair, 0)
    lax.fori_loop(NEXP - 2, NEXP, up1_one, 0)

    wait_all(hbuf.at[pl.ds(0, 2), pl.ds(0, 7)], xsend.at[0])
    wait_all(meta.at[pl.ds(1, 7)], msend.at[0])

    def d_copy(cb, g):
        return remote(hbuf.at[cb, g], drecv.at[cb, g], d_send.at[0], d_recv.at[cb] if g else d_stay.at[0], 0, 1)

    def s2_copy(cb, h):
        return remote(hbuf.at[cb, 3, pl.ds(h * TOK, TOK)], r2.at[cb, pl.ds(h * TOK, TOK)],
                      s2_send.at[0], s2_recv.at[cb // 2], HOP1[h], 0)

    def s3_copy(i, h):
        return remote(hbuf.at[pl.ds(2 * i, 2), 2, pl.ds(h * TOK + HALF, HALF)],
                      r3.at[pl.ds(2 * i, 2), pl.ds(h * HALF, HALF)],
                      s3_send.at[0], s3_recv.at[(i + 1) // (NCB // 2)], HOP2[h], 0)

    def part(cb):
        slot = lax.rem(N13 + cb, NSLOT)
        wait_w(slot)
        for e in range(NEXP):
            o = jnp.dot(act[e], wcols(slot, e), preferred_element_type=F32).astype(BF16)
            for c in range(4):
                obuf[c, 2 * CAP * e:2 * CAP * (e + 1), :] = o[2 * CAP * c:2 * CAP * (c + 1)]
        for c in (3, 1, 2, 0):
            t = jnp.dot(gmat[c], obuf[c], preferred_element_type=F32)
            t = t[0:128] + t[128:256] + t[256:384]
            for h in range(2):
                g = 0 if c in STAY[h] else 1
                place = (LEAVE if g else STAY)[h].index(c)
                at = pl.ds(h * TOK + place * HALF, HALF)
                hbuf[cb, 2 + g, at] = t[h * HALF:(h + 1) * HALF]
                hbuf[cb, g, at] = t[TOK + h * HALF:TOK + (h + 1) * HALF]
        d_copy(cb, 1).start()
        d_copy(cb, 0).start()

    def stage2(cb):
        d_copy(cb, 1).wait_recv()
        hbuf[cb, 3] = hbuf[cb, 3] + drecv[cb, 1]
        s2_copy(cb, 0).start()
        s2_copy(cb, 1).start()

    def down(cb, carry):
        part(cb)

        @pl.when(cb > 0)
        def _():
            stage2(cb - 1)

        return carry

    lax.fori_loop(0, NCB, down, 0)
    stage2(NCB - 1)

    wait_all(drecv.at[:, 0], d_stay.at[0])

    def third(i, carry):
        pair = pl.ds(2 * i, 2)
        wait_all(r2.at[pair], s2_recv.at[i])
        hbuf[pair, 2] = (hbuf[pair, 2] + drecv[pair, 0]) + r2[pair]
        for h in range(2):
            s3_copy(i, h).start()
        return carry

    lax.fori_loop(0, NCB // 2, third, 0)
    wait_all(drecv, d_send.at[0])
    wait_all(r2, s2_send.at[0])

    def last(cb, carry):
        cols = pl.ds(pl.multiple_of(lax.rem(cb, 4) * CB, CB), CB)
        ycols = pl.ds(pl.multiple_of(cb * CB, CB), CB)
        for h in range(2):
            at = pl.ds(h * HALF, HALF)
            xin = xs[cb // 4, 0, at, cols].astype(F32)
            y_ref[at, ycols] = (xin + (hbuf[cb, 2, pl.ds(h * TOK, HALF)] + r3[cb, at])).astype(BF16)
        return carry

    wait_all(r3.at[pl.ds(0, NCB - 2)], s3_recv.at[0])
    lax.fori_loop(0, NCB - 2, last, 0)
    wait_all(r3.at[pl.ds(NCB - 2, 2)], s3_recv.at[1])
    lax.fori_loop(NCB - 2, NCB, last, 0)
    wait_all(r3, s3_send.at[0])


def solution(mesh):
    def local_layer(x_loc, ids_loc, gates_loc, w_g, w_u, w_d):
        w_g = w_g.reshape(NEXP, 2, FFN, FFN)
        w_u = w_u.reshape(NEXP, 2, FFN, FFN)
        any_spec = pl.BlockSpec(memory_space=pl.ANY)
        dma = pltpu.SemaphoreType.DMA
        return pl.pallas_call(
            kernel,
            out_shape=pltpu.VMEM((TOK, HID), BF16),
            in_specs=[any_spec] * 6,
            out_specs=pl.BlockSpec(memory_space=pltpu.VMEM),
            scratch_shapes=[
                pltpu.VMEM((NSLOT, NEXP, FFN, CB), BF16),
                pltpu.VMEM((2, 4, 2 * TOK, FFN), BF16),
                pltpu.VMEM((2, NEXP, 8 * CAP, FFN), BF16),
                pltpu.VMEM((NEXP, 8, 8 * CAP, CB), F32),
                pltpu.VMEM((NEXP, 8 * CAP, FFN), BF16),
                pltpu.VMEM((NCB, 2, 2 * TOK, CB), F32),
                pltpu.VMEM((NCB, 2 * TOK, CB), F32),
                pltpu.VMEM((NCB, TOK, CB), F32),
                pltpu.VMEM((4, 2 * CAP * NEXP, 128), BF16),
                pltpu.VMEM((4, 2 * CAP * NEXP, 128), F32),
                pltpu.VMEM((4, 384, 2 * CAP * NEXP), BF16),
                pltpu.VMEM((4, 2 * CAP * NEXP, CB), BF16),
                pltpu.VMEM((8, TOK), jnp.int32),
                pltpu.VMEM((8, TOK), F32),
                pltpu.VMEM((8, 8, 128), F32),
                dma((NSLOT,)),
                dma((4,)),
                dma((1,)),
                dma((2, 2, 2)),
                dma((2, 2)),
                dma((2, 2, 2)),
                dma((2, 2)),
                dma((1,)),
                dma((1,)),
                dma((1,)),
                dma((NCB,)),
                dma((1,)),
                dma((1,)),
                dma((NCB // 2,)),
                dma((1,)),
                dma((2,)),
            ],
            compiler_params=pltpu.CompilerParams(collective_id=0, has_side_effects=True,
                                                 vmem_limit_bytes=66000000),
            name='moe_decode',
        )(x_loc, ids_loc.T, gates_loc.T, w_g, w_u, w_d)

    tok_spec = P(TOKEN_AXES, None)
    w_spec = P(EXPERT_AXES, None, None)
    return jax.shard_map(local_layer, mesh=mesh, in_specs=(tok_spec, tok_spec, tok_spec, w_spec, w_spec, w_spec), out_specs=tok_spec, check_vma=False)
```
